32 devices in a mesh: dp: 16 (over z, y, core), tensor: 2 (over x).
Axes of the slice: x: 2, y: 2, z: 4, core: 2. Of those that a mesh axis runs over, the one named last changes fastest.
Arguments:
- noisy_sample: float32 [2048, 28], P('dp'), may hold values from -5 to 5
- timestep: int32 [2048], P('dp'), may hold values from 0 to 99
- noise: float32 [2048, 28], P('dp'), may hold values from -5 to 5
- obs_feat: bfloat16 [2048, 1024], P('dp'), may hold values from -6 to 6
- step_w1: bfloat16 [256, 1024], replicated, may hold values from -0.75 to 0.75
- step_w2: bfloat16 [1024, 256], replicated, may hold values from -0.25 to 0.25
- film_weight: bfloat16 [1280, 2, 4096], P('dp', None, 'tensor'), may hold values from -0.25 to 0.25
- conv_in_w: bfloat16 [5, 7, 4096], P(None, None, 'tensor'), may hold values from -1 to 1
- residual_w: bfloat16 [7, 4096], P(None, 'tensor'), may hold values from -2 to 2
- conv_mid_w: bfloat16 [5, 4096, 4096], P(None, 'dp', 'tensor'), may hold values from -0.0390625 to 0.0390625
- out_w: bfloat16 [4096, 7], P('tensor'), may hold values from -0.1875 to 0.1875
- gain_one: float32 [4096], P('tensor'), may hold values from 0.4 to 1.6
- gain_two: float32 [4096], P('tensor'), may hold values from 0.4 to 1.6
Outputs:
- predicted_noise: float32 [2048, 28], P('dp')
- denoised: float32 [2048, 28], P('dp')
The draws below stay inside these ranges and needn't reach their ends.
All inputs are finite; a program needn't handle non-finite values.
Results may differ from the reference program's by a relative error of at most 0.0046.
Values may be sent and summed in bfloat16 or wider, within the bound.
A program may use at most 192 MiB of HBM per device.

```python
import math
import jax
import jax.numpy as jnp
from jax import lax

C = 4096
ACT = 7
HORIZON = 4
TAPS = 5
GROUPS = 8
STEP = 256
STEP_HID = 1024
OBS_FEAT = 1024
TRAIN_STEPS = 100
COND = 1280
OBS = 2048


def set_ends(result, rng, smallest, largest):
    longest = result.shape.index(max(result.shape))
    spots = []
    for shift in (0, 1):
        where = [jax.random.randint(jax.random.fold_in(rng, axis), (), 0, length) for axis, length in enumerate(result.shape)]
        where[longest] = (where[longest] + shift) % result.shape[longest]
        spots.append(tuple(where))
    return result.at[spots[0]].set(smallest).at[spots[1]].set(largest)


def levels(key, shape, shards, smallest, largest):
    loudness, own = 1.0, jax.random.fold_in(key, 6)
    for axis_at, blocks in shards:
        heights = jnp.exp(jax.random.uniform(jax.random.fold_in(own, axis_at), (blocks,), jnp.float32, smallest / len(shards), largest / len(shards)))
        loudness = loudness * jnp.repeat(heights, shape[axis_at] // blocks).reshape([-1 if axis == axis_at else 1 for axis in range(len(shape))])
    return loudness


def scatter_about(own_key, dims, scale, bound, cuts=(), kind=jnp.bfloat16):
    values = scale * jax.random.normal(own_key, dims, jnp.float32)
    if cuts:
        values = values * levels(own_key, dims, cuts, -0.22, 0.18)
    return jnp.clip(values, -bound, bound).astype(kind)


def setup_inputs(seed: int = 0) -> dict:
    streams_of = jax.random.split(jax.random.key(seed), 14)
    noisy_sample = scatter_about(streams_of[0], (OBS, HORIZON * ACT), 1.0, 5.0, ((0, 16),), jnp.float32)
    timestep = set_ends(jax.random.randint(streams_of[1], (OBS,), 0, TRAIN_STEPS), jax.random.fold_in(streams_of[1], 1), 0, TRAIN_STEPS - 1).astype(jnp.int32)
    noise = scatter_about(streams_of[2], (OBS, HORIZON * ACT), 1.0, 5.0, ((0, 16),), jnp.float32)
    obs_feat = scatter_about(streams_of[3], (OBS, OBS_FEAT), 1.0, 6.0, ((0, 16),))
    step_w1 = scatter_about(streams_of[4], (STEP, STEP_HID), (STEP // 4) ** -0.5, 0.75)
    step_w2 = scatter_about(streams_of[5], (STEP_HID, STEP), (STEP_HID // 2) ** -0.5, 0.25)
    film_weight = scatter_about(streams_of[6], (COND, 2, C), (COND // 2) ** -0.5, 0.25, ((0, 16), (2, 2)))
    conv_in_w = scatter_about(streams_of[7], (TAPS, ACT, C), (TAPS * ACT) ** -0.5, 1.0, ((2, 2),))
    residual_w = scatter_about(streams_of[8], (ACT, C), ACT ** -0.5, 2.0, ((1, 2),))
    conv_mid_w = scatter_about(streams_of[9], (TAPS, C, C), (TAPS * C) ** -0.5, 0.0390625, ((1, 16), (2, 2)))
    out_w = scatter_about(streams_of[10], (C, ACT), (C // 4) ** -0.5, 0.1875, ((0, 2),))
    gain_one = jnp.clip(0.4 + 1.2 * jax.random.uniform(streams_of[11], (C,), jnp.float32) ** levels(streams_of[11], (C,), ((0, 2),), -0.2, 0.2), 0.4, 1.6)
    gain_two = jnp.clip(0.4 + 1.2 * jax.random.uniform(streams_of[12], (C,), jnp.float32) ** levels(streams_of[12], (C,), ((0, 2),), -0.2, 0.2), 0.4, 1.6)
    return dict(noisy_sample=noisy_sample, timestep=timestep, noise=noise, obs_feat=obs_feat, step_w1=step_w1, step_w2=step_w2, film_weight=film_weight, conv_in_w=conv_in_w, residual_w=residual_w, conv_mid_w=conv_mid_w, out_w=out_w, gain_one=gain_one, gain_two=gain_two)


def plan():
    pos = jnp.arange(TRAIN_STEPS + 1, dtype=jnp.float32) / TRAIN_STEPS
    curve = jnp.cos((pos + 0.008) / 1.008 * (math.pi / 2)) ** 2
    betas = jnp.minimum(1.0 - curve[1:] / curve[:-1], 0.999)
    return jnp.cumprod(1.0 - betas)

def lookup(table, steps):
    onehot = (steps[:, None] == jnp.arange(table.shape[0], dtype=jnp.int32)[None, :]).astype(jnp.float32)
    return lax.optimization_barrier(jnp.sum(onehot * table[None, :], axis=1))

def mish(value):
    return value * jnp.tanh(jax.nn.softplus(value))

def sinusoid(steps):
    half = STEP // 2
    freqs = jnp.exp(jnp.arange(half, dtype=jnp.float32) * (-math.log(10000.0) / (half - 1)))
    angles = steps.astype(jnp.float32)[:, None] * freqs[None, :]
    return jnp.concatenate([jnp.sin(angles), jnp.cos(angles)], axis=1)

def convolve(acts, weight):
    count, length, inner = acts.shape
    padded = jnp.pad(acts, ((0, 0), (2, 2), (0, 0)))
    total = jnp.zeros((count * length, weight.shape[2]), jnp.float32)
    for shift in range(TAPS):
        window = padded[:, shift:shift + length, :].reshape(count * length, inner)
        total = total + jnp.dot(window, weight[shift], preferred_element_type=jnp.float32)
    return total.reshape(count, length, weight.shape[2])

def group_norm(hidden, gain, groups):
    count, length, width = hidden.shape
    split = hidden.reshape(count, length, groups, width // groups)
    mean = lax.optimization_barrier(jnp.mean(split, axis=(1, 3), keepdims=True))
    var = lax.optimization_barrier(jnp.mean((split - mean) ** 2, axis=(1, 3), keepdims=True))
    normed = ((split - mean) / jnp.sqrt(var + 1e-05)).reshape(count, length, width)
    return normed * gain[None, None, :]

def denoise_step(sample, eps, noise, steps):
    alpha_bar = plan()
    now = lookup(alpha_bar, steps)[:, None]
    before = jnp.where(steps > 0, lookup(alpha_bar, jnp.maximum(steps - 1, 0)), 1.0)[:, None]
    beta_prod = 1.0 - now
    cur_alpha = now / before
    cur_beta = 1.0 - cur_alpha
    start = jnp.clip((sample - jnp.sqrt(beta_prod) * eps) / jnp.sqrt(now), -1.0, 1.0)
    mean = jnp.sqrt(before) * cur_beta / beta_prod * start + jnp.sqrt(cur_alpha) * (1.0 - before) / beta_prod * sample
    spread = jnp.sqrt((1.0 - before) / beta_prod * cur_beta)
    return mean + spread * noise

def reference(noisy_sample, timestep, noise, obs_feat, step_w1, step_w2, film_weight, conv_in_w, residual_w, conv_mid_w, out_w, gain_one, gain_two):
    count = noisy_sample.shape[0]
    sample_b = noisy_sample.reshape(count, HORIZON, ACT).astype(jnp.bfloat16)
    sinus = sinusoid(timestep).astype(jnp.bfloat16)
    step_hidden = mish(jnp.dot(sinus, step_w1, preferred_element_type=jnp.float32)).astype(jnp.bfloat16)
    step_feat = jnp.dot(step_hidden, step_w2, preferred_element_type=jnp.float32)
    cond = mish(jnp.concatenate([step_feat, obs_feat.astype(jnp.float32)], axis=1)).astype(jnp.bfloat16)
    film = jnp.dot(cond, film_weight.reshape(COND, 2 * C), preferred_element_type=jnp.float32)
    scale = film[:, :C]
    shift = film[:, C:]
    first = mish(group_norm(convolve(sample_b, conv_in_w), gain_one, GROUPS))
    act_one = (scale[:, None, :] * first + shift[:, None, :]).astype(jnp.bfloat16)
    skip = jnp.dot(sample_b.reshape(count * HORIZON, ACT), residual_w, preferred_element_type=jnp.float32).reshape(count, HORIZON, C)
    act_two = (mish(group_norm(convolve(act_one, conv_mid_w), gain_two, GROUPS)) + skip).astype(jnp.bfloat16)
    eps = jnp.dot(act_two.reshape(count * HORIZON, C), out_w, preferred_element_type=jnp.float32).reshape(count, HORIZON * ACT)
    denoised = denoise_step(noisy_sample, eps, noise, timestep)
    return (eps, denoised)
```

```python
import math

import jax
import jax.numpy as jnp
from jax import lax
from jax.experimental import pallas as pl
from jax.experimental.pallas import tpu as pltpu
from jax.sharding import Mesh
from jax.sharding import PartitionSpec as P

C = 4096
ACT = 7
HORIZON = 4
TAPS = 5
GROUPS = 8
STEP = 256
TRAIN_STEPS = 100


def plan():
    pos = jnp.arange(TRAIN_STEPS + 1, dtype=jnp.float32) / TRAIN_STEPS
    curve = jnp.cos((pos + 0.008) / 1.008 * (math.pi / 2)) ** 2
    betas = jnp.minimum(1.0 - curve[1:] / curve[:-1], 0.999)
    return jnp.cumprod(1.0 - betas)


def lookup(table, steps):
    onehot = (steps[:, None] == jnp.arange(table.shape[0], dtype=jnp.int32)[None, :]).astype(
        jnp.float32
    )
    return jnp.sum(onehot * table[None, :], axis=1)


def mish(value):
    e = jnp.exp(jnp.minimum(value, 20.0))
    n = e * (e + 2.0)
    return value * (n / (n + 2.0))


def sinusoid(steps):
    half = STEP // 2
    freqs = jnp.exp(jnp.arange(half, dtype=jnp.float32) * (-math.log(10000.0) / (half - 1)))
    angles = steps.astype(jnp.float32)[:, None] * freqs[None, :]
    return jnp.concatenate([jnp.sin(angles), jnp.cos(angles)], axis=1)


def denoise_step(sample, eps, noise, steps):
    alpha_bar = plan()
    now = lookup(alpha_bar, steps)[:, None]
    before = jnp.where(steps > 0, lookup(alpha_bar, jnp.maximum(steps - 1, 0)), 1.0)[:, None]
    beta_prod = 1.0 - now
    cur_alpha = now / before
    cur_beta = 1.0 - cur_alpha
    start = jnp.clip((sample - jnp.sqrt(beta_prod) * eps) / jnp.sqrt(now), -1.0, 1.0)
    mean = (
        jnp.sqrt(before) * cur_beta / beta_prod * start
        + jnp.sqrt(cur_alpha) * (1.0 - before) / beta_prod * sample
    )
    spread = jnp.sqrt((1.0 - before) / beta_prod * cur_beta)
    return mean + spread * noise


DEPTH_PARTS = 4
PARTS = 2
VMEM = 60 * 1024 * 1024


def first_kernel(blocks, x_ref, wt_ref, cond_ref, film_ref, gain_ref, out_ref):
    x = x_ref[...]
    hs = [
        jnp.dot(x, wt_ref[h], preferred_element_type=jnp.float32) for h in range(HORIZON)
    ]
    width = hs[0].shape[1]
    count = HORIZON * width
    mean = sum(jnp.sum(h, axis=1, keepdims=True) for h in hs) / count
    hs = [h - mean for h in hs]
    var = sum(jnp.sum(h * h, axis=1, keepdims=True) for h in hs) / count
    inv = 1.0 / jnp.sqrt(var + 1e-05)
    cond = cond_ref[...]
    scale = jnp.dot(cond, film_ref[0], preferred_element_type=jnp.float32)
    shift = jnp.dot(cond, film_ref[1], preferred_element_type=jnp.float32)
    gain = gain_ref[...]
    cl = width // blocks
    for h in range(HORIZON):
        val = (scale * mish(hs[h] * inv * gain) + shift).astype(jnp.bfloat16)
        for b in range(blocks):
            out_ref[b, :, h * cl : (h + 1) * cl] = val[:, b * cl : (b + 1) * cl]


def first_stage(xs, wt, cond, film, gain, blocks, cl):
    rows = xs.shape[0]
    width = wt.shape[2]
    gw = C // GROUPS
    per = gw // cl
    rt = min(128, rows)
    inner = cond.shape[1]
    kern = lambda *refs: first_kernel(per, *refs)
    return pl.pallas_call(
        kern,
        grid=(width // gw, rows // rt),
        in_specs=[
            pl.BlockSpec((rt, xs.shape[1]), lambda g, r: (r, 0)),
            pl.BlockSpec((HORIZON, wt.shape[1], gw), lambda g, r: (0, 0, g)),
            pl.BlockSpec((rt, inner), lambda g, r: (r, 0)),
            pl.BlockSpec((2, inner, gw), lambda g, r: (0, 0, g)),
            pl.BlockSpec((1, gw), lambda g, r: (0, g)),
        ],
        out_specs=pl.BlockSpec((per, rt, HORIZON * cl), lambda g, r: (g, r, 0)),
        out_shape=jax.ShapeDtypeStruct((blocks, rows, HORIZON * cl), jnp.bfloat16),
        compiler_params=pltpu.CompilerParams(vmem_limit_bytes=VMEM),
        cost_estimate=pl.CostEstimate(
            flops=4 * rows * inner * width,
            bytes_accessed=4 * inner * width + 2 * rows * width * HORIZON,
            transcendentals=rows * width * HORIZON,
        ),
        name="first_stage",
    )(xs, wt, cond, film, gain)


def mix_kernel(pieces, mid, order_ref, *refs):
    a_ref, w_refs, out_ref = refs[0], refs[1 : 1 + pieces], refs[1 + pieces]
    cl = w_refs[0].shape[0] // TAPS
    parts, _, rows, _ = out_ref.shape
    for h in range(HORIZON):
        p0 = max(0, h - mid)
        p1 = min(HORIZON, h - mid + TAPS)
        k0 = p0 - h + mid
        k1 = p1 - h + mid
        acc = None
        for i in range(pieces):
            left = a_ref[order_ref[i], :, p0 * cl : p1 * cl]
            term = jnp.dot(
                left, w_refs[i][k0 * cl : k1 * cl, :], preferred_element_type=jnp.float32
            )
            acc = term if acc is None else acc + term
        for q in range(parts):
            out_ref[q, h] = acc[q * rows : (q + 1) * rows].astype(jnp.bfloat16)


def mix(order, acts, pieces):
    n = len(pieces)
    rows = acts.shape[1]
    width = pieces[0].shape[1]
    nt = min(256, width)
    kern = lambda *refs: mix_kernel(n, TAPS // 2, *refs)
    return pl.pallas_call(
        kern,
        grid=(width // nt,),
        in_specs=[
            pl.BlockSpec(memory_space=pltpu.SMEM),
            pl.BlockSpec(acts.shape, lambda j: (0, 0, 0)),
        ]
        + [pl.BlockSpec((p.shape[0], nt), lambda j: (0, j)) for p in pieces],
        out_specs=pl.BlockSpec(
            (DEPTH_PARTS, HORIZON, rows // DEPTH_PARTS, nt), lambda j: (0, 0, 0, j)
        ),
        out_shape=jax.ShapeDtypeStruct(
            (DEPTH_PARTS, HORIZON, rows // DEPTH_PARTS, width), jnp.bfloat16
        ),
        compiler_params=pltpu.CompilerParams(vmem_limit_bytes=VMEM),
        cost_estimate=pl.CostEstimate(
            flops=2 * 14 * rows * n * pieces[0].shape[0] // TAPS * width,
            bytes_accessed=2 * n * pieces[0].shape[0] * width + 8 * rows * width,
            transcendentals=0,
        ),
        name="mix",
    )(order, acts, *pieces)


def hop(value, axis, step):
    size = lax.axis_size(axis)
    return lax.ppermute(value, axis, [(i, (i + step) % size) for i in range(size)])


def relative(value):
    return jnp.concatenate(
        [value] + [hop(value, "z", -q) for q in range(1, DEPTH_PARTS)], axis=0
    )


def reduce_parts(part):
    half = HORIZON // 2
    far = part[2]
    up = hop(far[:half], "z", 1)
    down = hop(far[half:], "z", -1)
    f32 = jnp.float32
    near_up = (part[1, :half].astype(f32) + up.astype(f32)).astype(jnp.bfloat16)
    near_down = (part[3, half:].astype(f32) + down.astype(f32)).astype(jnp.bfloat16)
    got = [
        (hop(near_up, "z", 1), hop(part[3, :half], "z", -1)),
        (hop(part[1, half:], "z", 1), hop(near_down, "z", -1)),
    ]
    out = []
    for h in range(HORIZON):
        one, two = got[h // half]
        out.append(
            part[0, h].astype(f32) + one[h % half].astype(f32) + two[h % half].astype(f32)
        )
    return out


def general_body(
    noisy_sample,
    timestep,
    noise,
    obs_feat,
    step_w1,
    step_w2,
    film_weight,
    conv_in_w,
    residual_w,
    conv_mid_w,
    out_w,
    gain_one,
    gain_two,
):
    count = noisy_sample.shape[0]
    local_width = conv_in_w.shape[2]
    cl = conv_mid_w.shape[1]
    yn = lax.axis_size("y")
    zi, yi, ci = lax.axis_index("z"), lax.axis_index("y"), lax.axis_index("c")
    blocks = yn * 2
    kw = cl * blocks
    step = local_width // PARTS
    pieces = []
    for n in range(PARTS):
        own = conv_mid_w.reshape(TAPS * cl, local_width)[:, n * step : (n + 1) * step]
        near = [own] + [hop(own, "y", -s) for s in range(1, yn)]
        pieces.append(near + [hop(v, "c", 1) for v in near])
    order = jnp.stack(
        [((yi + s) % yn) * 2 + ci for s in range(yn)]
        + [((yi + s) % yn) * 2 + (1 - ci) for s in range(yn)]
    ).astype(jnp.int32)
    film = jnp.transpose(film_weight, (1, 0, 2))
    film = lax.all_gather(film, "tensor", axis=2, tiled=True)
    film = lax.all_to_all(film, "z", split_axis=2, concat_axis=1, tiled=True)
    film = lax.all_gather(film, ("y", "c"), axis=1, tiled=True)
    win = lax.all_gather(conv_in_w, "tensor", axis=2, tiled=True)
    win = lax.dynamic_slice_in_dim(win, zi * kw, kw, 2)
    gain = lax.all_gather(gain_one, "tensor", axis=0, tiled=True)
    gain = lax.dynamic_slice_in_dim(gain, zi * kw, kw, 0)[None, :]
    toep = []
    for h in range(HORIZON):
        rows = []
        for p in range(HORIZON):
            k = p - h + TAPS // 2
            rows.append(win[k] if 0 <= k < TAPS else jnp.zeros((ACT, kw), win.dtype))
        toep.append(jnp.concatenate(rows, axis=0))
    toep = jnp.stack(toep)
    sample_b = noisy_sample.astype(jnp.bfloat16)
    sinus = sinusoid(timestep).astype(jnp.bfloat16)
    step_hidden = mish(jnp.dot(sinus, step_w1, preferred_element_type=jnp.float32)).astype(
        jnp.bfloat16
    )
    step_feat = jnp.dot(step_hidden, step_w2, preferred_element_type=jnp.float32)
    cond = mish(jnp.concatenate([step_feat, obs_feat.astype(jnp.float32)], axis=1)).astype(
        jnp.bfloat16
    )
    fr = film_weight.shape[0]
    cond = (
        cond.reshape(count, DEPTH_PARTS, blocks, fr)
        .transpose(0, 2, 1, 3)
        .reshape(count, cond.shape[1])
    )
    acts = first_stage(relative(sample_b), toep, relative(cond), film, gain, blocks, cl)
    found = [reduce_parts(mix(order, acts, p)) for p in pieces]
    hs = [jnp.concatenate([f[h] for f in found], axis=1) for h in range(HORIZON)]
    gw = C // GROUPS
    outs = []
    cols = [slice(g * gw, (g + 1) * gw) for g in range(local_width // gw)]
    stats = []
    for col in cols:
        mean = sum(jnp.sum(h[:, col], axis=1, keepdims=True) for h in hs) / (HORIZON * gw)
        var = sum(jnp.sum((h[:, col] - mean) ** 2, axis=1, keepdims=True) for h in hs) / (
            HORIZON * gw
        )
        stats.append((mean, 1.0 / jnp.sqrt(var + 1e-05)))
    mean = jnp.concatenate([jnp.broadcast_to(m, (count, gw)) for m, _ in stats], axis=1)
    inv = jnp.concatenate([jnp.broadcast_to(v, (count, gw)) for _, v in stats], axis=1)
    for h in range(HORIZON):
        skip = jnp.dot(
            sample_b[:, h * ACT : (h + 1) * ACT], residual_w, preferred_element_type=jnp.float32
        )
        normed = (hs[h] - mean) * inv * gain_two[None, :]
        act_two = (mish(normed) + skip).astype(jnp.bfloat16)
        outs.append(jnp.dot(act_two, out_w, preferred_element_type=jnp.float32))
    eps = lax.psum(jnp.concatenate(outs, axis=1), "tensor")
    denoised = denoise_step(noisy_sample, eps, noise, timestep)
    return (eps, denoised)


CHUNK = 256
SPLIT = 2
LANES = 128
MESH_ID = pl.DeviceIdType.MESH


def remote(src, dst, send, recv, where):
    return pltpu.make_async_remote_copy(
        src_ref=src,
        dst_ref=dst,
        send_sem=send,
        recv_sem=recv,
        device_id=where,
        device_id_type=MESH_ID,
    )


def normed(hs, gain):
    count = len(hs) * hs[0].shape[1]
    mean = sum(jnp.sum(h, axis=1, keepdims=True) for h in hs) / count
    hs = [h - mean for h in hs]
    var = sum(jnp.sum(h * h, axis=1, keepdims=True) for h in hs) / count
    inv = 1.0 / jnp.sqrt(var + 1e-05)
    return [h * inv * gain for h in hs]


def fused_kernel(
    sinus_ref,
    obs_ref,
    samp_ref,
    w1_ref,
    w2_ref,
    film_ref,
    toep_ref,
    gain_one_ref,
    mid_ref,
    res_ref,
    outw_ref,
    gain_two_ref,
    eps_ref,
    w_buf,
    a_buf,
    film_buf,
    cond_buf,
    toep_buf,
    gain_buf,
    own_part,
    z_recv,
    z_send,
    last,
    eps_acc,
    eps_send,
    eps_recv,
    own_sem,
    core_send,
    core_recv,
    y_send,
    y_recv,
    fwd_send,
    fwd_recv,
    film_send,
    film_recv,
    filmy_sem,
    filmx_send,
    filmx_recv,
    filmc_send,
    filmc_recv,
    toep_send,
    toep_recv,
    cond_send,
    cond_recv,
    condx_send,
    condx_recv,
    zs_sem,
    zr_sem,
    eps_ssem,
    eps_rsem,
):
    zi, yi = lax.axis_index("z"), lax.axis_index("y")
    ci, xi = lax.axis_index("c"), lax.axis_index("tensor")
    zn = DEPTH_PARTS
    f32, b16 = jnp.float32, jnp.bfloat16
    chunks = w_buf.shape[0]
    cl = w_buf.shape[2] // TAPS
    rows = eps_ref.shape[0]
    gw = C // GROUPS
    width = mid_ref.shape[1]
    kw = film_buf.shape[5]
    feat = w2_ref.shape[1] + obs_ref.shape[1]
    mid = TAPS // 2
    oy, oc, ox = 1 - yi, 1 - ci, 1 - xi
    to_y, to_c, to_x = {"y": oy}, {"c": oc}, {"tensor": ox}

    barrier = pltpu.get_barrier_semaphore()
    peers = [to_y, to_c]
    for dz in range(zn):
        for dx in range(2):
            if dz or dx:
                peers.append({"z": lax.rem(zi + dz, zn), "tensor": lax.rem(xi + dx, 2)})
    for peer in peers:
        pl.semaphore_signal(barrier, inc=1, device_id=peer, device_id_type=MESH_ID)

    def cols(j):
        return pl.ds(pl.multiple_of(j * CHUNK, CHUNK), CHUNK)

    def own_copy(j):
        return pltpu.make_async_copy(mid_ref.at[:, cols(j)], w_buf.at[j, 0], own_sem.at[j])

    def core_copy(j):
        return remote(
            mid_ref.at[:, cols(j)], w_buf.at[j, 1], core_send.at[j], core_recv.at[j], to_c
        )

    def y_copy(j):
        return remote(mid_ref.at[:, cols(j)], w_buf.at[j, 2], y_send.at[j], y_recv.at[j], to_y)

    def fwd_copy(j):
        return remote(w_buf.at[j, 2], w_buf.at[j, 3], fwd_send.at[j], fwd_recv.at[j], to_c)

    def film_out(q, t):
        return remote(
            film_ref.at[t, :, pl.ds(q * kw, kw)],
            film_buf.at[t, zi, yi, ci],
            film_send.at[q, t],
            film_recv.at[zi],
            {"z": 2 * xi + q, "tensor": t},
        )

    pl.semaphore_wait(barrier, len(peers))
    y_copy(0).start()
    for q in range(2):
        for t in range(2):
            mine = (2 * xi + q == zi) & (xi == t)

            @pl.when(mine)
            def _():
                pltpu.make_async_copy(
                    film_ref.at[t, :, pl.ds(q * kw, kw)],
                    film_buf.at[t, zi, yi, ci],
                    film_recv.at[zi],
                ).start()

            @pl.when(jnp.logical_not(mine))
            def _():
                film_out(q, t).start()

    home = zi // 2
    at = pl.ds(pl.multiple_of(lax.rem(zi, 2) * kw, kw), kw)

    def toep_copy():
        return remote(
            toep_ref.at[:, :, at], toep_buf, toep_send.at[0], toep_recv.at[0], to_x
        )

    def gain_copy():
        return remote(gain_one_ref.at[:, at], gain_buf, toep_send.at[1], toep_recv.at[1], to_x)

    @pl.when(xi == home)
    def _():
        toep_copy().start()
        gain_copy().start()
        pltpu.make_async_copy(toep_ref.at[:, :, at], toep_buf, toep_recv.at[0]).start()
        pltpu.make_async_copy(gain_one_ref.at[:, at], gain_buf, toep_recv.at[1]).start()

    hidden = mish(jnp.dot(sinus_ref[...], w1_ref[...], preferred_element_type=f32)).astype(b16)
    step_feat = jnp.dot(hidden, w2_ref[...], preferred_element_type=f32)
    half = rows // 2
    sw = step_feat.shape[1]
    cond_step = mish(step_feat).astype(b16)
    cond_obs = mish(obs_ref[...].astype(f32)).astype(b16)
    for i in range(2):
        part = slice(i * half, (i + 1) * half)
        cond_buf[zi, i, :, :sw] = cond_step[part]
        cond_buf[zi, i, :, sw:feat] = cond_obs[part]
        cond_buf[zi, i, :, feat:] = samp_ref[part]

    def cond_copy(dz):
        return remote(
            cond_buf.at[zi, xi],
            cond_buf.at[zi, xi],
            cond_send.at[dz - 1],
            cond_recv.at[zi],
            {"z": lax.rem(zi + dz, zn)},
        )

    def condx_copy(z, i):
        return remote(
            cond_buf.at[z, i], cond_buf.at[z, i], condx_send.at[z], condx_recv.at[z], to_x
        )

    def cond_in(z):
        return remote(
            cond_buf.at[z, xi], cond_buf.at[z, xi], cond_send.at[0], cond_recv.at[z], to_x
        )

    for dz in range(1, zn):
        cond_copy(dz).start()

    @pl.loop(0, chunks)
    def _(j):
        own_copy(j).start()
        core_copy(j).start()

    def film_x(i, t, y):
        piece = film_buf.at[t, :, y, ci]
        return remote(piece, piece, filmx_send.at[i], filmx_recv.at[i], to_x)

    def film_y(y):
        piece = film_buf.at[xi, :, y, ci]
        return remote(piece, piece, filmy_sem.at[0], filmy_sem.at[1], to_y)

    def film_c(i, t, y, c):
        piece = film_buf.at[t, :, y, c]
        return remote(piece, piece, filmc_send.at[i], filmc_recv.at[i], to_c)

    for z in range(zn):
        piece = film_buf.at[xi, z, yi, ci]
        remote(piece, piece, film_send.at[0, 0], film_recv.at[z], to_x).wait_recv()
    film_y(yi).start()
    film_x(0, xi, yi).start()
    film_c(0, xi, yi, ci).start()

    @pl.loop(1, chunks)
    def _(j):
        y_copy(j).start()

    for dz in range(1, zn):
        z = lax.rem(zi + dz, zn)
        cond_in(z).wait_recv()
        condx_copy(z, xi).start()
    film_y(oy).wait_recv()
    film_x(1, xi, oy).start()
    film_c(1, xi, oy, ci).start()
    film_x(0, ox, yi).wait_recv()
    film_c(2, ox, yi, ci).start()
    film_x(1, ox, oy).wait_recv()
    film_c(3, ox, oy, ci).start()
    toep_copy().wait_recv()
    gain_copy().wait_recv()
    for dz in range(1, zn):
        condx_copy(lax.rem(zi + dz, zn), ox).wait_recv()
    for i, (t, y) in enumerate(((xi, yi), (xi, oy), (ox, yi), (ox, oy))):
        film_c(i, t, y, oc).wait_recv()

    per = gw // cl
    inner = film_buf.shape[1] * film_buf.shape[2] * film_buf.shape[3] * film_buf.shape[4]

    @pl.loop(0, zn)
    def _(z):
        cond = cond_buf[z].reshape(rows, cond_buf.shape[3])
        x = cond[:, feat : feat + toep_buf.shape[1]]
        cond = cond[:, :feat]
        ab = z // SPLIT
        r = lax.rem(z, SPLIT)
        for g in range(kw // gw):
            span = slice(g * gw, (g + 1) * gw)
            hs = [
                jnp.dot(x, toep_buf[h, :, span], preferred_element_type=f32)
                for h in range(HORIZON)
            ]
            hs = normed(hs, gain_buf[0:1, span])
            scale = jnp.dot(
                cond,
                film_buf[0, :, :, :, :, span].reshape(inner, gw),
                preferred_element_type=f32,
            )
            shift = jnp.dot(
                cond,
                film_buf[1, :, :, :, :, span].reshape(inner, gw),
                preferred_element_type=f32,
            )
            for h in range(HORIZON):
                val = (scale * mish(hs[h]) + shift).astype(b16)
                for b in range(per):
                    a_buf[g * per + b, r, ab, :, h * cl : (h + 1) * cl] = val[
                        :, b * cl : (b + 1) * cl
                    ]

    eps_acc[...] = jnp.zeros_like(eps_acc)
    order = [yi * 2 + ci, yi * 2 + oc, oy * 2 + ci, oy * 2 + oc]
    steps = chunks * SPLIT
    ring = own_part.shape[0]
    ends = (zi == 0) | (zi == zn - 1)

    def z_copy(d, s):
        k = lax.rem(s, ring)
        return remote(
            z_send.at[d, k],
            z_recv.at[d, s],
            zs_sem.at[d, k],
            zr_sem.at[d, s],
            {"z": jnp.maximum(zi - 1, 0) if d == 0 else jnp.minimum(zi + 1, zn - 1)},
        )

    def flow(d, now):
        lag = zn - 1 - zi if d == 0 else zi
        s = now - lag
        k = lax.rem(s + ring, ring)

        @pl.when((s >= 0) & (s < steps))
        def _():
            @pl.when(lag > 0)
            def _():
                z_copy(d, s).wait_recv()

            @pl.when(lag == zn - 1)
            def _():
                for h in range(HORIZON):
                    last[lax.rem(s, SPLIT), lax.rem(s // SPLIT, 2), h] = own_part[
                        k, d, h
                    ] + z_recv[d, s, h].astype(f32)

            @pl.when(lag < zn - 1)
            def _():
                @pl.when(s >= ring)
                def _():
                    z_copy(d, s - ring).wait_send()

                @pl.when(lag == 0)
                def _():
                    for h in range(HORIZON):
                        z_send[d, k, h] = own_part[k, d, h].astype(b16)

                @pl.when(lag > 0)
                def _():
                    for h in range(HORIZON):
                        z_send[d, k, h] = (
                            own_part[k, d, h] + z_recv[d, s, h].astype(f32)
                        ).astype(b16)

                z_copy(d, s).start()

    @pl.loop(0, steps + zn - 1)
    def _(now):
        @pl.when(now < steps)
        def _():
            j = now // SPLIT
            r = lax.rem(now, SPLIT)
            k = lax.rem(now, ring)

            @pl.when(r == 0)
            def _():
                y_copy(j).wait_recv()
                fwd_copy(j).start()
                own_copy(j).wait()
                core_copy(j).wait_recv()
                fwd_copy(j).wait_recv()

            for h in range(HORIZON):
                p0 = max(0, h - mid)
                p1 = min(HORIZON, h - mid + TAPS)
                k0 = p0 - h + mid
                k1 = p1 - h + mid
                acc = None
                for slot in range(4):
                    left = a_buf[order[slot], r, :, :, p0 * cl : p1 * cl]
                    term = jnp.dot(
                        left.reshape(2 * rows, (p1 - p0) * cl),
                        w_buf[j, slot, k0 * cl : k1 * cl, :],
                        preferred_element_type=f32,
                    )
                    acc = term if acc is None else acc + term
                for d in range(2):
                    own_part[k, d, h] = acc[d * rows : (d + 1) * rows]

        flow(1, now)
        flow(0, now)
        done = now - (zn - 1)

        @pl.when((done >= 0) & ends & (lax.rem(done // SPLIT, 2) == 1))
        def _():
            r = lax.rem(done, SPLIT)
            g = done // (2 * SPLIT)
            z = (zi // (zn - 1)) * SPLIT + r
            span = pl.ds(pl.multiple_of(g * gw, gw), gw)
            hs = [
                jnp.concatenate([last[r, 0, h], last[r, 1, h]], axis=1) for h in range(HORIZON)
            ]
            hs = normed(hs, gain_two_ref[0:1, span])
            x = cond_buf[z, :, :, feat:].reshape(rows, LANES)[:, : res_ref.shape[1]]
            for h in range(HORIZON):
                skip = jnp.dot(x, res_ref[h, :, span], preferred_element_type=f32)
                act = (mish(hs[h]) + skip).astype(b16)
                eps_acc[r, h] += jnp.dot(act, outw_ref[span, :], preferred_element_type=f32)

    end = (zi // SPLIT) * (zn - 1)

    def eps_copy(r, t):
        return remote(
            eps_send.at[r],
            eps_recv.at[xi],
            eps_ssem.at[r, t],
            eps_rsem.at[xi],
            {"z": (zi // (zn - 1)) * SPLIT + r, "tensor": t},
        )

    for r in range(SPLIT):
        z = (zi // (zn - 1)) * SPLIT + r

        @pl.when(ends)
        def _():
            total = eps_acc[r, 0]
            for h in range(1, HORIZON):
                total = total + pltpu.roll(eps_acc[r, h], h * ACT, 1)
            eps_send[r] = total

            @pl.when(z == zi)
            def _():
                eps_recv[xi] = total

            for t in range(2):

                @pl.when((z != zi) | (xi != t))
                def _():
                    eps_copy(r, t).start()

    for t in range(2):

        @pl.when((zi != end) | (xi != t))
        def _():
            remote(
                eps_send.at[0], eps_recv.at[t], eps_ssem.at[0, 0], eps_rsem.at[t], to_x
            ).wait_recv()

    eps_ref[...] = eps_recv[0] + eps_recv[1]

    for r in range(SPLIT):
        z = (zi // (zn - 1)) * SPLIT + r
        for t in range(2):

            @pl.when(ends & ((z != zi) | (xi != t)))
            def _():
                eps_copy(r, t).wait_send()

    for d in range(2):

        @pl.when((zi < zn - 1) if d else (zi > 0))
        def _():
            for s in range(steps - ring, steps):
                z_copy(d, s).wait_send()

    @pl.loop(0, chunks)
    def _(j):
        y_copy(j).wait_send()
        core_copy(j).wait_send()
        fwd_copy(j).wait_send()

    for q in range(2):
        for t in range(2):

            @pl.when((2 * xi + q != zi) | (xi != t))
            def _():
                film_out(q, t).wait_send()

    @pl.when(xi == home)
    def _():
        toep_copy().wait_send()
        gain_copy().wait_send()

    for dz in range(1, zn):
        cond_copy(dz).wait_send()
        condx_copy(lax.rem(zi + dz, zn), xi).wait_send()
    film_y(yi).wait_send()
    film_x(0, xi, yi).wait_send()
    film_x(1, xi, oy).wait_send()
    for i, (t, y) in enumerate(((xi, yi), (xi, oy), (ox, yi), (ox, oy))):
        film_c(i, t, y, ci).wait_send()


def fused(sinus, obs, samp, w1, w2, film, toep, gain_one, weights, res, outw, gain_two):
    rows = obs.shape[0]
    depth, width = weights.shape
    chunks = width // CHUNK
    cl = depth // TAPS
    kw = cl * 4
    fr = film.shape[1]
    feat = w2.shape[1] + obs.shape[1]
    steps = chunks * SPLIT
    ring = DEPTH_PARTS
    b16, f32 = jnp.bfloat16, jnp.float32
    dma = pltpu.SemaphoreType.DMA
    vm = pl.BlockSpec(memory_space=pltpu.VMEM)
    hbm = pl.BlockSpec(memory_space=pl.ANY)
    return pl.pallas_call(
        fused_kernel,
        out_shape=jax.ShapeDtypeStruct((rows, LANES), f32),
        in_specs=[vm, vm, vm, vm, vm, hbm, hbm, hbm, hbm, vm, vm, vm],
        out_specs=vm,
        scratch_shapes=[
            pltpu.VMEM((chunks, 4, depth, CHUNK), b16),
            pltpu.VMEM((4, SPLIT, 2, rows, HORIZON * cl), b16),
            pltpu.VMEM((2, DEPTH_PARTS, 2, 2, fr, kw), b16),
            pltpu.VMEM((DEPTH_PARTS, 2, rows // 2, feat + LANES), b16),
            pltpu.VMEM((HORIZON, toep.shape[1], kw), b16),
            pltpu.VMEM((gain_one.shape[0], kw), f32),
            pltpu.VMEM((ring, 2, HORIZON, rows, CHUNK), f32),
            pltpu.VMEM((2, steps, HORIZON, rows, CHUNK), b16),
            pltpu.VMEM((2, ring, HORIZON, rows, CHUNK), b16),
            pltpu.VMEM((SPLIT, 2, HORIZON, rows, CHUNK), f32),
            pltpu.VMEM((SPLIT, HORIZON, rows, LANES), f32),
            pltpu.VMEM((SPLIT, rows, LANES), f32),
            pltpu.VMEM((2, rows, LANES), f32),
            dma((chunks,)),
            dma((chunks,)),
            dma((chunks,)),
            dma((chunks,)),
            dma((chunks,)),
            dma((chunks,)),
            dma((chunks,)),
            dma((2, 2)),
            dma((DEPTH_PARTS,)),
            dma((2,)),
            dma((2,)),
            dma((2,)),
            dma((4,)),
            dma((4,)),
            dma((2,)),
            dma((2,)),
            dma((DEPTH_PARTS - 1,)),
            dma((DEPTH_PARTS,)),
            dma((DEPTH_PARTS,)),
            dma((DEPTH_PARTS,)),
            dma((2, ring)),
            dma((2, steps)),
            dma((SPLIT, 2)),
            dma((2,)),
        ],
        compiler_params=pltpu.CompilerParams(
            collective_id=0, has_side_effects=True, vmem_limit_bytes=VMEM
        ),
        name="fused_step",
    )(sinus, obs, samp, w1, w2, film, toep, gain_one, weights, res, outw, gain_two)


def spread(blocks, lead):
    width = next(b for b in blocks if b is not None).shape[1]
    rows = []
    for p in range(HORIZON):
        rows.append(blocks[p] if blocks[p] is not None else jnp.zeros((ACT, width), lead))
    rows.append(jnp.zeros((32 - HORIZON * ACT, width), lead))
    return jnp.concatenate(rows, axis=0)


def fused_body(
    noisy_sample,
    timestep,
    noise,
    obs_feat,
    step_w1,
    step_w2,
    film_weight,
    conv_in_w,
    residual_w,
    conv_mid_w,
    out_w,
    gain_one,
    gain_two,
):
    width = conv_in_w.shape[2]
    lead = conv_in_w.dtype
    taps = lambda h, p: p - h + TAPS // 2
    toep = jnp.stack(
        [
            spread(
                [
                    conv_in_w[taps(h, p)] if 0 <= taps(h, p) < TAPS else None
                    for p in range(HORIZON)
                ],
                lead,
            )
            for h in range(HORIZON)
        ]
    )
    blank = jnp.zeros((ACT, width), lead)
    res = jnp.stack(
        [
            spread([residual_w if p == h else blank for p in range(HORIZON)], lead)
            for h in range(HORIZON)
        ]
    )
    samp = jnp.pad(
        noisy_sample.astype(lead), ((0, 0), (0, LANES - noisy_sample.shape[1]))
    )
    eps = fused(
        sinusoid(timestep).astype(lead),
        obs_feat,
        samp,
        step_w1,
        step_w2,
        jnp.transpose(film_weight, (1, 0, 2)),
        toep,
        jnp.broadcast_to(gain_one[None, :], (8, width)),
        conv_mid_w.reshape(-1, width),
        res,
        jnp.pad(out_w, ((0, 0), (0, LANES - ACT))),
        gain_two[None, :],
    )[:, : HORIZON * ACT]
    return (eps, denoise_step(noisy_sample, eps, noise, timestep))


def solution(mesh):
    dp, tensor = mesh.shape["dp"], mesh.shape["tensor"]
    near = dp // DEPTH_PARTS // 2
    body = fused_body if near == 2 and tensor == 2 else general_body
    grid = Mesh(
        mesh.devices.reshape(DEPTH_PARTS, dp // DEPTH_PARTS // 2, 2, tensor),
        ("z", "y", "c", "tensor"),
    )
    rows = ("z", "y", "c")
    return jax.shard_map(
        body,
        mesh=grid,
        in_specs=(
            P(rows, None),
            P(rows),
            P(rows, None),
            P(rows, None),
            P(),
            P(),
            P(rows, None, "tensor"),
            P(None, None, "tensor"),
            P(None, "tensor"),
            P(None, rows, "tensor"),
            P("tensor", None),
            P("tensor"),
            P("tensor"),
        ),
        out_specs=(P(rows, None), P(rows, None)),
        check_vma=False,
    )
```

```python
import math

import jax
import jax.numpy as jnp
import numpy as np
from jax import lax
from jax.experimental import pallas as pl
from jax.experimental.pallas import tpu as pltpu
from jax.sharding import Mesh
from jax.sharding import PartitionSpec as P

C = 4096
ACT = 7
HORIZON = 4
TAPS = 5
GROUPS = 8
STEP = 256
TRAIN_STEPS = 100


def plan():
    pos = jnp.arange(TRAIN_STEPS + 1, dtype=jnp.float32) / TRAIN_STEPS
    curve = jnp.cos((pos + 0.008) / 1.008 * (math.pi / 2)) ** 2
    betas = jnp.minimum(1.0 - curve[1:] / curve[:-1], 0.999)
    return jnp.cumprod(1.0 - betas)


def lookup(table, steps):
    onehot = (steps[:, None] == jnp.arange(table.shape[0], dtype=jnp.int32)[None, :]).astype(
        jnp.float32
    )
    return jnp.sum(onehot * table[None, :], axis=1)


def mish(value):
    e = jnp.exp(jnp.minimum(value, 20.0))
    n = e * (e + 2.0)
    return value * (n / (n + 2.0))


def sinusoid(steps):
    half = STEP // 2
    freqs = jnp.exp(jnp.arange(half, dtype=jnp.float32) * (-math.log(10000.0) / (half - 1)))
    angles = steps.astype(jnp.float32)[:, None] * freqs[None, :]
    return jnp.concatenate([jnp.sin(angles), jnp.cos(angles)], axis=1)


def denoise_step(sample, eps, noise, steps):
    alpha_bar = plan()
    now = lookup(alpha_bar, steps)[:, None]
    before = jnp.where(steps > 0, lookup(alpha_bar, jnp.maximum(steps - 1, 0)), 1.0)[:, None]
    return denoise(sample, eps, noise, now, before)


def denoise(sample, eps, noise, now, before):
    beta_prod = 1.0 - now
    cur_alpha = now / before
    cur_beta = 1.0 - cur_alpha
    start = jnp.clip((sample - jnp.sqrt(beta_prod) * eps) / jnp.sqrt(now), -1.0, 1.0)
    mean = (
        jnp.sqrt(before) * cur_beta / beta_prod * start
        + jnp.sqrt(cur_alpha) * (1.0 - before) / beta_prod * sample
    )
    spread = jnp.sqrt((1.0 - before) / beta_prod * cur_beta)
    return mean + spread * noise


DEPTH_PARTS = 4
PARTS = 2
VMEM = 60 * 1024 * 1024


def first_kernel(blocks, x_ref, wt_ref, cond_ref, film_ref, gain_ref, out_ref):
    x = x_ref[...]
    hs = [
        jnp.dot(x, wt_ref[h], preferred_element_type=jnp.float32) for h in range(HORIZON)
    ]
    width = hs[0].shape[1]
    count = HORIZON * width
    mean = sum(jnp.sum(h, axis=1, keepdims=True) for h in hs) / count
    hs = [h - mean for h in hs]
    var = sum(jnp.sum(h * h, axis=1, keepdims=True) for h in hs) / count
    inv = 1.0 / jnp.sqrt(var + 1e-05)
    cond = cond_ref[...]
    scale = jnp.dot(cond, film_ref[0], preferred_element_type=jnp.float32)
    shift = jnp.dot(cond, film_ref[1], preferred_element_type=jnp.float32)
    gain = gain_ref[...]
    cl = width // blocks
    for h in range(HORIZON):
        val = (scale * mish(hs[h] * inv * gain) + shift).astype(jnp.bfloat16)
        for b in range(blocks):
            out_ref[b, :, h * cl : (h + 1) * cl] = val[:, b * cl : (b + 1) * cl]


def first_stage(xs, wt, cond, film, gain, blocks, cl):
    rows = xs.shape[0]
    width = wt.shape[2]
    gw = C // GROUPS
    per = gw // cl
    rt = min(128, rows)
    inner = cond.shape[1]
    kern = lambda *refs: first_kernel(per, *refs)
    return pl.pallas_call(
        kern,
        grid=(width // gw, rows // rt),
        in_specs=[
            pl.BlockSpec((rt, xs.shape[1]), lambda g, r: (r, 0)),
            pl.BlockSpec((HORIZON, wt.shape[1], gw), lambda g, r: (0, 0, g)),
            pl.BlockSpec((rt, inner), lambda g, r: (r, 0)),
            pl.BlockSpec((2, inner, gw), lambda g, r: (0, 0, g)),
            pl.BlockSpec((1, gw), lambda g, r: (0, g)),
        ],
        out_specs=pl.BlockSpec((per, rt, HORIZON * cl), lambda g, r: (g, r, 0)),
        out_shape=jax.ShapeDtypeStruct((blocks, rows, HORIZON * cl), jnp.bfloat16),
        compiler_params=pltpu.CompilerParams(vmem_limit_bytes=VMEM),
        cost_estimate=pl.CostEstimate(
            flops=4 * rows * inner * width,
            bytes_accessed=4 * inner * width + 2 * rows * width * HORIZON,
            transcendentals=rows * width * HORIZON,
        ),
        name="first_stage",
    )(xs, wt, cond, film, gain)


def mix_kernel(pieces, mid, order_ref, *refs):
    a_ref, w_refs, out_ref = refs[0], refs[1 : 1 + pieces], refs[1 + pieces]
    cl = w_refs[0].shape[0] // TAPS
    parts, _, rows, _ = out_ref.shape
    for h in range(HORIZON):
        p0 = max(0, h - mid)
        p1 = min(HORIZON, h - mid + TAPS)
        k0 = p0 - h + mid
        k1 = p1 - h + mid
        acc = None
        for i in range(pieces):
            left = a_ref[order_ref[i], :, p0 * cl : p1 * cl]
            term = jnp.dot(
                left, w_refs[i][k0 * cl : k1 * cl, :], preferred_element_type=jnp.float32
            )
            acc = term if acc is None else acc + term
        for q in range(parts):
            out_ref[q, h] = acc[q * rows : (q + 1) * rows].astype(jnp.bfloat16)


def mix(order, acts, pieces):
    n = len(pieces)
    rows = acts.shape[1]
    width = pieces[0].shape[1]
    nt = min(256, width)
    kern = lambda *refs: mix_kernel(n, TAPS // 2, *refs)
    return pl.pallas_call(
        kern,
        grid=(width // nt,),
        in_specs=[
            pl.BlockSpec(memory_space=pltpu.SMEM),
            pl.BlockSpec(acts.shape, lambda j: (0, 0, 0)),
        ]
        + [pl.BlockSpec((p.shape[0], nt), lambda j: (0, j)) for p in pieces],
        out_specs=pl.BlockSpec(
            (DEPTH_PARTS, HORIZON, rows // DEPTH_PARTS, nt), lambda j: (0, 0, 0, j)
        ),
        out_shape=jax.ShapeDtypeStruct(
            (DEPTH_PARTS, HORIZON, rows // DEPTH_PARTS, width), jnp.bfloat16
        ),
        compiler_params=pltpu.CompilerParams(vmem_limit_bytes=VMEM),
        cost_estimate=pl.CostEstimate(
            flops=2 * 14 * rows * n * pieces[0].shape[0] // TAPS * width,
            bytes_accessed=2 * n * pieces[0].shape[0] * width + 8 * rows * width,
            transcendentals=0,
        ),
        name="mix",
    )(order, acts, *pieces)


def hop(value, axis, step):
    size = lax.axis_size(axis)
    return lax.ppermute(value, axis, [(i, (i + step) % size) for i in range(size)])


def relative(value):
    return jnp.concatenate(
        [value] + [hop(value, "z", -q) for q in range(1, DEPTH_PARTS)], axis=0
    )


def reduce_parts(part):
    half = HORIZON // 2
    far = part[2]
    up = hop(far[:half], "z", 1)
    down = hop(far[half:], "z", -1)
    f32 = jnp.float32
    near_up = (part[1, :half].astype(f32) + up.astype(f32)).astype(jnp.bfloat16)
    near_down = (part[3, half:].astype(f32) + down.astype(f32)).astype(jnp.bfloat16)
    got = [
        (hop(near_up, "z", 1), hop(part[3, :half], "z", -1)),
        (hop(part[1, half:], "z", 1), hop(near_down, "z", -1)),
    ]
    out = []
    for h in range(HORIZON):
        one, two = got[h // half]
        out.append(
            part[0, h].astype(f32) + one[h % half].astype(f32) + two[h % half].astype(f32)
        )
    return out


def general_body(
    noisy_sample,
    timestep,
    noise,
    obs_feat,
    step_w1,
    step_w2,
    film_weight,
    conv_in_w,
    residual_w,
    conv_mid_w,
    out_w,
    gain_one,
    gain_two,
):
    count = noisy_sample.shape[0]
    local_width = conv_in_w.shape[2]
    cl = conv_mid_w.shape[1]
    yn = lax.axis_size("y")
    zi, yi, ci = lax.axis_index("z"), lax.axis_index("y"), lax.axis_index("c")
    blocks = yn * 2
    kw = cl * blocks
    step = local_width // PARTS
    pieces = []
    for n in range(PARTS):
        own = conv_mid_w.reshape(TAPS * cl, local_width)[:, n * step : (n + 1) * step]
        near = [own] + [hop(own, "y", -s) for s in range(1, yn)]
        pieces.append(near + [hop(v, "c", 1) for v in near])
    order = jnp.stack(
        [((yi + s) % yn) * 2 + ci for s in range(yn)]
        + [((yi + s) % yn) * 2 + (1 - ci) for s in range(yn)]
    ).astype(jnp.int32)
    film = jnp.transpose(film_weight, (1, 0, 2))
    film = lax.all_gather(film, "tensor", axis=2, tiled=True)
    film = lax.all_to_all(film, "z", split_axis=2, concat_axis=1, tiled=True)
    film = lax.all_gather(film, ("y", "c"), axis=1, tiled=True)
    win = lax.all_gather(conv_in_w, "tensor", axis=2, tiled=True)
    win = lax.dynamic_slice_in_dim(win, zi * kw, kw, 2)
    gain = lax.all_gather(gain_one, "tensor", axis=0, tiled=True)
    gain = lax.dynamic_slice_in_dim(gain, zi * kw, kw, 0)[None, :]
    toep = []
    for h in range(HORIZON):
        rows = []
        for p in range(HORIZON):
            k = p - h + TAPS // 2
            rows.append(win[k] if 0 <= k < TAPS else jnp.zeros((ACT, kw), win.dtype))
        toep.append(jnp.concatenate(rows, axis=0))
    toep = jnp.stack(toep)
    sample_b = noisy_sample.astype(jnp.bfloat16)
    sinus = sinusoid(timestep).astype(jnp.bfloat16)
    step_hidden = mish(jnp.dot(sinus, step_w1, preferred_element_type=jnp.float32)).astype(
        jnp.bfloat16
    )
    step_feat = jnp.dot(step_hidden, step_w2, preferred_element_type=jnp.float32)
    cond = mish(jnp.concatenate([step_feat, obs_feat.astype(jnp.float32)], axis=1)).astype(
        jnp.bfloat16
    )
    fr = film_weight.shape[0]
    cond = (
        cond.reshape(count, DEPTH_PARTS, blocks, fr)
        .transpose(0, 2, 1, 3)
        .reshape(count, cond.shape[1])
    )
    acts = first_stage(relative(sample_b), toep, relative(cond), film, gain, blocks, cl)
    found = [reduce_parts(mix(order, acts, p)) for p in pieces]
    hs = [jnp.concatenate([f[h] for f in found], axis=1) for h in range(HORIZON)]
    gw = C // GROUPS
    outs = []
    cols = [slice(g * gw, (g + 1) * gw) for g in range(local_width // gw)]
    stats = []
    for col in cols:
        mean = sum(jnp.sum(h[:, col], axis=1, keepdims=True) for h in hs) / (HORIZON * gw)
        var = sum(jnp.sum((h[:, col] - mean) ** 2, axis=1, keepdims=True) for h in hs) / (
            HORIZON * gw
        )
        stats.append((mean, 1.0 / jnp.sqrt(var + 1e-05)))
    mean = jnp.concatenate([jnp.broadcast_to(m, (count, gw)) for m, _ in stats], axis=1)
    inv = jnp.concatenate([jnp.broadcast_to(v, (count, gw)) for _, v in stats], axis=1)
    for h in range(HORIZON):
        skip = jnp.dot(
            sample_b[:, h * ACT : (h + 1) * ACT], residual_w, preferred_element_type=jnp.float32
        )
        normed = (hs[h] - mean) * inv * gain_two[None, :]
        act_two = (mish(normed) + skip).astype(jnp.bfloat16)
        outs.append(jnp.dot(act_two, out_w, preferred_element_type=jnp.float32))
    eps = lax.psum(jnp.concatenate(outs, axis=1), "tensor")
    denoised = denoise_step(noisy_sample, eps, noise, timestep)
    return (eps, denoised)


CHUNK = 256
SPLIT = 2
LANES = 128
MESH_ID = pl.DeviceIdType.MESH


def remote(src, dst, send, recv, where):
    return pltpu.make_async_remote_copy(
        src_ref=src,
        dst_ref=dst,
        send_sem=send,
        recv_sem=recv,
        device_id=where,
        device_id_type=MESH_ID,
    )


def normed(hs, gain):
    count = len(hs) * hs[0].shape[1]
    mean = sum(jnp.sum(h, axis=1, keepdims=True) for h in hs) / count
    hs = [h - mean for h in hs]
    var = sum(jnp.sum(h * h, axis=1, keepdims=True) for h in hs) / count
    inv = 1.0 / jnp.sqrt(var + 1e-05)
    return [h * inv * gain for h in hs]


def fused_kernel(
    steps_ref,
    obs_ref,
    samp_ref,
    w1_ref,
    w2_ref,
    film_ref,
    conv_ref,
    gain_one_ref,
    mid_ref,
    skip_ref,
    outw_ref,
    gain_two_ref,
    sel_ref,
    noise_ref,
    table_ref,
    out_ref,
    square,
    w_buf,
    a_buf,
    film_buf,
    stage_buf,
    cond_buf,
    conv_buf,
    toep_buf,
    res_buf,
    gain_buf,
    own_part,
    z_recv,
    z_send,
    last,
    eps_acc,
    eps_send,
    eps_recv,
    own_sem,
    core_send,
    core_recv,
    y_send,
    y_recv,
    fwd_send,
    fwd_recv,
    stage_send,
    stage_recv,
    film_send,
    film_recv,
    filmy_send,
    filmy_recv,
    filmx_send,
    filmx_recv,
    filmc_send,
    filmc_recv,
    toep_send,
    toep_recv,
    cond_send,
    cond_recv,
    pair_send,
    pair_recv,
    condx_send,
    condx_recv,
    zs_sem,
    zr_sem,
    eps_ssem,
    eps_rsem,
):
    zi, yi = lax.axis_index("z"), lax.axis_index("y")
    ci, xi = lax.axis_index("c"), lax.axis_index("tensor")
    zn = DEPTH_PARTS
    f32, b16 = jnp.float32, jnp.bfloat16
    chunks = w_buf.shape[0]
    cl = w_buf.shape[2] // TAPS
    rows = obs_ref.shape[0]
    gw = C // GROUPS
    width = mid_ref.shape[1]
    kw = film_buf.shape[5]
    feat = w2_ref.shape[1] + obs_ref.shape[1]
    mid = TAPS // 2
    oy, oc, ox = 1 - yi, 1 - ci, 1 - xi
    to_y, to_c, to_x = {"y": oy}, {"c": oc}, {"tensor": ox}

    barrier = pltpu.get_barrier_semaphore()
    peers = [to_y, to_c]
    for dz in range(zn):
        for dx in range(2):
            if dz or dx:
                peers.append({"z": lax.rem(zi + dz, zn), "tensor": lax.rem(xi + dx, 2)})
    for peer in peers:
        pl.semaphore_signal(barrier, inc=1, device_id=peer, device_id_type=MESH_ID)

    def cols(j):
        return pl.ds(pl.multiple_of(j * CHUNK, CHUNK), CHUNK)

    def own_copy(j):
        return pltpu.make_async_copy(mid_ref.at[:, cols(j)], w_buf.at[j, 0], own_sem.at[j])

    def core_copy(j):
        return remote(
            mid_ref.at[:, cols(j)], w_buf.at[j, 1], core_send.at[j], core_recv.at[j], to_c
        )

    def y_half(j, i):
        some = pl.ds(i * (w_buf.shape[2] // 2), w_buf.shape[2] // 2)
        return remote(
            mid_ref.at[some, cols(j)],
            w_buf.at[j, 2, some],
            y_send.at[j, i],
            y_recv.at[j, i],
            to_y,
        )

    def fwd_copy(j):
        return remote(w_buf.at[j, 2], w_buf.at[j, 3], fwd_send.at[j], fwd_recv.at[j], to_c)

    near = [zi, zi + 1 - 2 * lax.rem(zi, 2), lax.rem(zi + 2, zn), zn - 1 - zi]
    home = zi // 2

    def half_cols(q):
        return pl.ds(pl.multiple_of(q * kw, kw), kw)

    def stage_copy(q):
        return remote(
            film_ref.at[ox, :, half_cols(q)],
            stage_buf.at[q],
            stage_send.at[q],
            stage_recv.at[q],
            to_x,
        )

    def plane_copy():
        return remote(
            film_ref.at[ox, :, half_cols(lax.rem(zi, 2))],
            film_buf.at[ox, zi, yi, ci],
            stage_send.at[lax.rem(zi, 2)],
            film_recv.at[zi],
            to_x,
        )

    def film_own(q):
        return remote(
            film_ref.at[xi, :, half_cols(q)],
            film_buf.at[xi, zi, yi, ci],
            film_send.at[0, q],
            film_recv.at[zi],
            {"z": 2 * xi + q},
        )

    def film_staged(q):
        return remote(
            stage_buf.at[q],
            film_buf.at[xi, zi, yi, ci],
            film_send.at[1, q],
            film_recv.at[zi],
            {"z": 2 * ox + q},
        )

    pl.semaphore_wait(barrier, len(peers))
    for q in range(2):
        mine = 2 * xi + q == zi

        @pl.when(mine)
        def _():
            plane_copy().start()
            pltpu.make_async_copy(
                film_ref.at[xi, :, half_cols(q)], film_buf.at[xi, zi, yi, ci], film_recv.at[zi]
            ).start()

        @pl.when(jnp.logical_not(mine))
        def _():
            stage_copy(q).start()
            film_own(q).start()

    y_half(0, 0).start()

    at = half_cols(lax.rem(zi, 2))

    def conv_copy():
        return remote(conv_ref.at[:, :, at], conv_buf, toep_send.at[0], toep_recv.at[0], to_x)

    def gain_copy():
        return remote(gain_one_ref.at[:, at], gain_buf, toep_send.at[1], toep_recv.at[1], to_x)

    @pl.when(xi == home)
    def _():
        conv_copy().start()
        gain_copy().start()
        pltpu.make_async_copy(conv_ref.at[:, :, at], conv_buf, toep_recv.at[0]).start()
        pltpu.make_async_copy(gain_one_ref.at[:, at], gain_buf, toep_recv.at[1]).start()

    half = rows // 2
    sw = w2_ref.shape[1]
    cond_obs = mish(obs_ref[...].astype(f32)).astype(b16)
    square[...] = jnp.zeros_like(square)
    square[: HORIZON * ACT] = samp_ref[...]
    samp = square[...].T.astype(b16)
    count = w1_ref.shape[0] // 2
    index = lax.broadcasted_iota(jnp.int32, (count, rows), 0).astype(f32)
    freqs = jnp.exp(index * (-math.log(10000.0) / (count - 1)))
    angles = steps_ref[...].astype(f32) * freqs
    sinus = jnp.concatenate([jnp.sin(angles), jnp.cos(angles)], axis=0).astype(b16)
    hidden = mish(
        lax.dot_general(
            sinus, w1_ref[...], (((0,), (0,)), ((), ())), preferred_element_type=f32
        )
    ).astype(b16)
    step_feat = jnp.dot(hidden, w2_ref[...], preferred_element_type=f32)
    cond_step = mish(step_feat).astype(b16)
    for i in range(2):
        part = slice(i * half, (i + 1) * half)
        cond_buf[zi, i, :, :sw] = cond_step[part]
        cond_buf[zi, i, :, sw:feat] = cond_obs[part]
        cond_buf[zi, i, :, feat:] = samp[part]

    def cond_copy(dz):
        return remote(
            cond_buf.at[zi, xi],
            cond_buf.at[zi, xi],
            cond_send.at[dz - 2],
            cond_recv.at[zi],
            {"z": near[dz]},
        )

    def condx_copy(z, i):
        return remote(
            cond_buf.at[z, i], cond_buf.at[z, i], condx_send.at[z], condx_recv.at[z], to_x
        )

    def cond_in(z):
        return remote(
            cond_buf.at[z, xi], cond_buf.at[z, xi], cond_send.at[0], cond_recv.at[z], to_x
        )

    for q in range(2):

        @pl.when(2 * ox + q != zi)
        def _():
            stage_copy(q).wait_recv()
            film_staged(q).start()

    def cond_pair(i):
        return remote(
            cond_buf.at[zi, i],
            cond_buf.at[zi, i],
            pair_send.at[i],
            pair_recv.at[i],
            {"z": near[1]},
        )

    for i in range(2):
        cond_pair(i).start()
    for k in range(2, zn):
        cond_copy(k).start()

    @pl.loop(0, chunks)
    def _(j):
        own_copy(j).start()
        core_copy(j).start()

    def film_in(z):
        piece = film_buf.at[xi, z, yi, ci]
        return remote(piece, piece, film_send.at[0, 0], film_recv.at[z], to_x)

    def film_y(z, t, y):
        piece = film_buf.at[t, z, y, ci]
        return remote(piece, piece, filmy_send.at[z], filmy_recv.at[z], to_y)

    def film_x(z, t, y):
        piece = film_buf.at[t, z, y, ci]
        k = (y + yi) % 2
        return remote(piece, piece, filmx_send.at[k, z], filmx_recv.at[k, z], to_x)

    def film_c(z, t, y, c):
        piece = film_buf.at[t, z, y, c]
        k = 2 * ((t + xi) % 2) + (y + yi) % 2
        return remote(piece, piece, filmc_send.at[k, z], filmc_recv.at[k, z], to_c)

    def arrived(z):
        film_in(z).wait_recv()
        film_y(z, xi, yi).start()
        film_x(z, xi, yi).start()
        film_c(z, xi, yi, ci).start()

    def crossed(z):
        film_y(z, xi, oy).wait_recv()
        film_x(z, xi, oy).start()
        film_c(z, xi, oy, ci).start()

    def known(z):
        cond_in(z).wait_recv()
        condx_copy(z, xi).start()

    arrived(near[0])
    y_half(0, 1).start()
    arrived(near[1])
    crossed(near[0])
    arrived(near[2])
    crossed(near[1])
    y_half(1, 0).start()
    arrived(near[3])
    y_half(1, 1).start()
    crossed(near[2])

    @pl.loop(2, chunks)
    def _(j):
        for i in range(2):
            y_half(j, i).start()

    known(near[2])
    crossed(near[3])
    known(near[3])
    conv_copy().wait_recv()
    gain_copy().wait_recv()
    total = None
    for k in range(TAPS):
        term = jnp.dot(sel_ref[k], conv_buf[k], preferred_element_type=f32)
        total = term if total is None else total + term
    toep_buf[...] = total.astype(b16)
    res_buf[...] = jnp.dot(sel_ref[mid], skip_ref[...], preferred_element_type=f32).astype(b16)
    for z in near:
        film_x(z, ox, yi).wait_recv()
        film_c(z, ox, yi, ci).start()
    for z in near:
        film_x(z, ox, oy).wait_recv()
        film_c(z, ox, oy, ci).start()
    for z in near[2:]:
        condx_copy(z, ox).wait_recv()
    for i in range(2):
        piece = cond_buf.at[near[1], i]
        remote(piece, piece, pair_send.at[i], pair_recv.at[i], to_x).wait_recv()
    for z in near:
        for t in range(2):
            for y in range(2):
                film_c(z, t, y, oc).wait_recv()

    per = gw // cl
    inner = film_buf.shape[1] * film_buf.shape[2] * film_buf.shape[3] * film_buf.shape[4]
    pad = sel_ref.shape[1] // HORIZON

    def first(r, ab):
        z = ab * SPLIT + r
        cond = cond_buf[z].reshape(rows, cond_buf.shape[3])
        x = cond[:, feat : feat + pad]
        cond = cond[:, :feat]
        for g in range(kw // gw):
            span = slice(g * gw, (g + 1) * gw)
            hs = [
                jnp.dot(
                    x, toep_buf[h * pad : (h + 1) * pad, span], preferred_element_type=f32
                )
                for h in range(HORIZON)
            ]
            hs = normed(hs, gain_buf[0:1, span])
            scale = jnp.dot(
                cond,
                film_buf[0, :, :, :, :, span].reshape(inner, gw),
                preferred_element_type=f32,
            )
            shift = jnp.dot(
                cond,
                film_buf[1, :, :, :, :, span].reshape(inner, gw),
                preferred_element_type=f32,
            )
            for h in range(HORIZON):
                val = (scale * mish(hs[h]) + shift).astype(b16)
                for b in range(per):
                    a_buf[g * per + b, r, ab, :, h * cl : (h + 1) * cl] = val[
                        :, b * cl : (b + 1) * cl
                    ]

    eps_acc[...] = jnp.zeros_like(eps_acc)
    order = [yi * 2 + ci, yi * 2 + oc, oy * 2 + ci, oy * 2 + oc]
    steps = chunks * SPLIT
    ring = own_part.shape[0]
    zring = z_send.shape[1]
    ends = (zi == 0) | (zi == zn - 1)

    def z_copy(d, s, h):
        k = lax.rem(s, zring)
        return remote(
            z_send.at[d, k, h],
            z_recv.at[d, s, h],
            zs_sem.at[d, k, h],
            zr_sem.at[d, s, h],
            {"z": jnp.maximum(zi - 1, 0) if d == 0 else jnp.minimum(zi + 1, zn - 1)},
        )

    def flow(d, now):
        pos = zn - 1 - zi if d == 0 else zi
        s = now - pos - pos // (zn - 1)
        k = lax.rem(s + ring, ring)
        kz = lax.rem(s + zring, zring)

        @pl.when((s >= 0) & (s < steps))
        def _():
            @pl.when(pos == zn - 1)
            def _():
                for h in range(HORIZON):
                    z_copy(d, s, h).wait_recv()
                    last[lax.rem(s, SPLIT), lax.rem(s // SPLIT, 2), h] = own_part[
                        k, d, h
                    ] + z_recv[d, s, h].astype(f32)

            @pl.when((pos < zn - 1) & (s >= zring))
            def _():
                for h in range(HORIZON):
                    z_copy(d, s - zring, h).wait_send()

            @pl.when(pos == 0)
            def _():
                for h in range(HORIZON):
                    z_send[d, kz, h] = own_part[k, d, h].astype(b16)
                    z_copy(d, s, h).start()

            @pl.when((pos > 0) & (pos < zn - 1))
            def _():
                for h in range(HORIZON):
                    z_copy(d, s, h).wait_recv()
                    z_send[d, kz, h] = (
                        own_part[k, d, h] + z_recv[d, s, h].astype(f32)
                    ).astype(b16)
                    z_copy(d, s, h).start()

    @pl.loop(0, steps + zn)
    def _(now):
        @pl.when(now < SPLIT)
        def _():
            @pl.loop(0, 2)
            def _(ab):
                first(now, ab)

        @pl.when(now < steps)
        def _():
            j = now // SPLIT
            r = lax.rem(now, SPLIT)
            k = lax.rem(now, ring)

            @pl.when(r == 0)
            def _():
                for i in range(2):
                    y_half(j, i).wait_recv()
                fwd_copy(j).start()
                own_copy(j).wait()
                core_copy(j).wait_recv()
                fwd_copy(j).wait_recv()

            for h in range(HORIZON):
                p0 = max(0, h - mid)
                p1 = min(HORIZON, h - mid + TAPS)
                k0 = p0 - h + mid
                k1 = p1 - h + mid
                acc = None
                for slot in range(4):
                    left = a_buf[order[slot], r, :, :, p0 * cl : p1 * cl]
                    term = jnp.dot(
                        left.reshape(2 * rows, (p1 - p0) * cl),
                        w_buf[j, slot, k0 * cl : k1 * cl, :],
                        preferred_element_type=f32,
                    )
                    acc = term if acc is None else acc + term
                for d in range(2):
                    own_part[k, d, h] = acc[d * rows : (d + 1) * rows]

        flow(1, now)
        flow(0, now)
        done = now - zn

        @pl.when((done >= 0) & ends & (lax.rem(done // SPLIT, 2) == 1))
        def _():
            r = lax.rem(done, SPLIT)
            g = done // (2 * SPLIT)
            z = (zi // (zn - 1)) * SPLIT + r
            span = pl.ds(pl.multiple_of(g * gw, gw), gw)
            hs = [
                jnp.concatenate([last[r, 0, h], last[r, 1, h]], axis=1) for h in range(HORIZON)
            ]
            hs = normed(hs, gain_two_ref[0:1, span])
            x = cond_buf[z, :, :, feat:].reshape(rows, LANES)[:, :pad]
            for h in range(HORIZON):
                skip = jnp.dot(
                    x, res_buf[h * pad : (h + 1) * pad, span], preferred_element_type=f32
                )
                act = (mish(hs[h]) + skip).astype(b16)
                eps_acc[r, h] += lax.dot_general(
                    act,
                    outw_ref[:, span],
                    (((1,), (1,)), ((), ())),
                    preferred_element_type=f32,
                )

    end = (zi // SPLIT) * (zn - 1)

    def eps_copy(r, t):
        return remote(
            eps_send.at[r],
            eps_recv.at[xi],
            eps_ssem.at[r, t],
            eps_rsem.at[xi],
            {"z": (zi // (zn - 1)) * SPLIT + r, "tensor": t},
        )

    for r in range(SPLIT):
        z = (zi // (zn - 1)) * SPLIT + r

        @pl.when(ends)
        def _():
            total = jnp.concatenate(
                [eps_acc[r, h] for h in range(HORIZON)]
                + [jnp.zeros((rows, LANES - HORIZON * ACT), f32)],
                axis=1,
            )
            total = total.T[: eps_send.shape[1]]
            eps_send[r] = total

            @pl.when(z == zi)
            def _():
                eps_recv[xi] = total

            for t in range(2):

                @pl.when((z != zi) | (xi != t))
                def _():
                    eps_copy(r, t).start()

    for t in range(2):

        @pl.when((zi != end) | (xi != t))
        def _():
            remote(
                eps_send.at[0], eps_recv.at[t], eps_ssem.at[0, 0], eps_rsem.at[t], to_x
            ).wait_recv()

    eps = (eps_recv[0] + eps_recv[1])[: HORIZON * ACT]
    out_ref[0, : HORIZON * ACT] = eps
    when = steps_ref[...]
    spots = lax.broadcasted_iota(jnp.int32, square.shape, 0)
    table = jnp.broadcast_to(table_ref[...], square.shape).T
    now = jnp.sum(jnp.where(spots == when, table, 0.0), axis=0, keepdims=True)
    before = jnp.sum(jnp.where(spots == when - 1, table, 0.0), axis=0, keepdims=True)
    before = jnp.where(when > 0, before, 1.0)
    out_ref[1, : HORIZON * ACT] = denoise(samp_ref[...], eps, noise_ref[...], now, before)

    for r in range(SPLIT):
        z = (zi // (zn - 1)) * SPLIT + r
        for t in range(2):

            @pl.when(ends & ((z != zi) | (xi != t)))
            def _():
                eps_copy(r, t).wait_send()

    for d in range(2):

        @pl.when((zi < zn - 1) if d else (zi > 0))
        def _():
            for s in range(steps - zring, steps):
                for h in range(HORIZON):
                    z_copy(d, s, h).wait_send()

    @pl.loop(0, chunks)
    def _(j):
        for i in range(2):
            y_half(j, i).wait_send()
        core_copy(j).wait_send()
        fwd_copy(j).wait_send()

    for q in range(2):
        mine = 2 * xi + q == zi

        @pl.when(mine)
        def _():
            plane_copy().wait_send()

        @pl.when(jnp.logical_not(mine))
        def _():
            stage_copy(q).wait_send()
            film_own(q).wait_send()

        @pl.when(2 * ox + q != zi)
        def _():
            film_staged(q).wait_send()

    @pl.when(xi == home)
    def _():
        conv_copy().wait_send()
        gain_copy().wait_send()

    for i in range(2):
        cond_pair(i).wait_send()
    for k in range(2, zn):
        cond_copy(k).wait_send()
        condx_copy(near[k], xi).wait_send()
    for z in near:
        film_y(z, xi, yi).wait_send()
        film_x(z, xi, yi).wait_send()
        film_x(z, xi, oy).wait_send()
        for y in range(2):
            for t in range(2):
                film_c(z, t, y, ci).wait_send()


def fused(steps, obs, samp, w1, w2, film, conv, gain_one, weights, skip, outw, gain_two, sel, noise, table):
    rows = obs.shape[0]
    depth, width = weights.shape
    chunks = width // CHUNK
    cl = depth // TAPS
    kw = cl * 4
    fr = film.shape[1]
    feat = w2.shape[1] + obs.shape[1]
    count = chunks * SPLIT
    ring = DEPTH_PARTS + 1
    zring = 4
    b16, f32 = jnp.bfloat16, jnp.float32
    dma = pltpu.SemaphoreType.DMA
    vm = pl.BlockSpec(memory_space=pltpu.VMEM)
    hbm = pl.BlockSpec(memory_space=pl.ANY)
    return pl.pallas_call(
        fused_kernel,
        out_shape=jax.ShapeDtypeStruct((2, 32, rows), f32),
        in_specs=[vm, vm, vm, vm, vm, hbm, hbm, hbm, hbm, vm, vm, vm, vm, vm, vm],
        out_specs=vm,
        scratch_shapes=[
            pltpu.VMEM((LANES, LANES), f32),
            pltpu.VMEM((chunks, 4, depth, CHUNK), b16),
            pltpu.VMEM((4, SPLIT, 2, rows, HORIZON * cl), b16),
            pltpu.VMEM((2, DEPTH_PARTS, 2, 2, fr, kw), b16),
            pltpu.VMEM((2, fr, kw), b16),
            pltpu.VMEM((DEPTH_PARTS, 2, rows // 2, feat + LANES), b16),
            pltpu.VMEM((TAPS, ACT, kw), b16),
            pltpu.VMEM((sel.shape[1], kw), b16),
            pltpu.VMEM((sel.shape[1], width), b16),
            pltpu.VMEM((gain_one.shape[0], kw), f32),
            pltpu.VMEM((ring, 2, HORIZON, rows, CHUNK), f32),
            pltpu.VMEM((2, count, HORIZON, rows, CHUNK), b16),
            pltpu.VMEM((2, zring, HORIZON, rows, CHUNK), b16),
            pltpu.VMEM((SPLIT, 2, HORIZON, rows, CHUNK), f32),
            pltpu.VMEM((SPLIT, HORIZON, rows, ACT), f32),
            pltpu.VMEM((SPLIT, 32, rows), f32),
            pltpu.VMEM((2, 32, rows), f32),
            dma((chunks,)),
            dma((chunks,)),
            dma((chunks,)),
            dma((chunks, 2)),
            dma((chunks, 2)),
            dma((chunks,)),
            dma((chunks,)),
            dma((2,)),
            dma((2,)),
            dma((2, 2)),
            dma((DEPTH_PARTS,)),
            dma((DEPTH_PARTS,)),
            dma((DEPTH_PARTS,)),
            dma((2, DEPTH_PARTS)),
            dma((2, DEPTH_PARTS)),
            dma((4, DEPTH_PARTS)),
            dma((4, DEPTH_PARTS)),
            dma((2,)),
            dma((2,)),
            dma((DEPTH_PARTS - 2,)),
            dma((DEPTH_PARTS,)),
            dma((2,)),
            dma((2,)),
            dma((DEPTH_PARTS,)),
            dma((DEPTH_PARTS,)),
            dma((2, zring, HORIZON)),
            dma((2, count, HORIZON)),
            dma((SPLIT, 2)),
            dma((2,)),
        ],
        compiler_params=pltpu.CompilerParams(
            collective_id=0, has_side_effects=True, vmem_limit_bytes=VMEM
        ),
        name="fused_step",
    )(steps, obs, samp, w1, w2, film, conv, gain_one, weights, skip, outw, gain_two, sel, noise, table)


def selection(dtype):
    pad = 32
    table = np.zeros((TAPS, HORIZON * pad, ACT), np.float32)
    for h in range(HORIZON):
        for p in range(HORIZON):
            k = p - h + TAPS // 2
            for a in range(ACT):
                if 0 <= k < TAPS:
                    table[k, h * pad + p * ACT + a, a] = 1.0
    return jnp.asarray(table, dtype)


def fused_body(
    noisy_sample,
    timestep,
    noise,
    obs_feat,
    step_w1,
    step_w2,
    film_weight,
    conv_in_w,
    residual_w,
    conv_mid_w,
    out_w,
    gain_one,
    gain_two,
):
    width = conv_in_w.shape[2]
    table = plan()
    both = fused(
        timestep[None, :],
        obs_feat,
        noisy_sample.T,
        step_w1,
        step_w2,
        jnp.transpose(film_weight, (1, 0, 2)),
        conv_in_w,
        gain_one[None, :],
        conv_mid_w.reshape(-1, width),
        residual_w,
        out_w.T,
        gain_two[None, :],
        selection(conv_in_w.dtype),
        noise.T,
        jnp.pad(table, (0, LANES - table.shape[0]))[None, :],
    )
    return (both[0, : HORIZON * ACT].T, both[1, : HORIZON * ACT].T)


def solution(mesh):
    dp, tensor = mesh.shape["dp"], mesh.shape["tensor"]
    near = dp // DEPTH_PARTS // 2
    body = fused_body if near == 2 and tensor == 2 else general_body
    grid = Mesh(
        mesh.devices.reshape(DEPTH_PARTS, dp // DEPTH_PARTS // 2, 2, tensor),
        ("z", "y", "c", "tensor"),
    )
    rows = ("z", "y", "c")
    return jax.shard_map(
        body,
        mesh=grid,
        in_specs=(
            P(rows, None),
            P(rows),
            P(rows, None),
            P(rows, None),
            P(),
            P(),
            P(rows, None, "tensor"),
            P(None, None, "tensor"),
            P(None, "tensor"),
            P(None, rows, "tensor"),
            P("tensor", None),
            P("tensor"),
            P("tensor"),
        ),
        out_specs=(P(rows, None), P(rows, None)),
        check_vma=False,
    )
```

```python
import math

import jax
import jax.numpy as jnp
import numpy as np
from jax import lax
from jax.experimental import pallas as pl
from jax.experimental.pallas import tpu as pltpu
from jax.sharding import Mesh
from jax.sharding import PartitionSpec as P

C = 4096
ACT = 7
HORIZON = 4
TAPS = 5
GROUPS = 8
STEP = 256
TRAIN_STEPS = 100


def plan():
    pos = jnp.arange(TRAIN_STEPS + 1, dtype=jnp.float32) / TRAIN_STEPS
    curve = jnp.cos((pos + 0.008) / 1.008 * (math.pi / 2)) ** 2
    betas = jnp.minimum(1.0 - curve[1:] / curve[:-1], 0.999)
    return jnp.cumprod(1.0 - betas)


def lookup(table, steps):
    onehot = (steps[:, None] == jnp.arange(table.shape[0], dtype=jnp.int32)[None, :]).astype(
        jnp.float32
    )
    return jnp.sum(onehot * table[None, :], axis=1)


def mish(value):
    e = jnp.exp(jnp.minimum(value, 20.0))
    n = e * (e + 2.0)
    return value * (n / (n + 2.0))


def sinusoid(steps):
    half = STEP // 2
    freqs = jnp.exp(jnp.arange(half, dtype=jnp.float32) * (-math.log(10000.0) / (half - 1)))
    angles = steps.astype(jnp.float32)[:, None] * freqs[None, :]
    return jnp.concatenate([jnp.sin(angles), jnp.cos(angles)], axis=1)


def denoise_step(sample, eps, noise, steps):
    alpha_bar = plan()
    now = lookup(alpha_bar, steps)[:, None]
    before = jnp.where(steps > 0, lookup(alpha_bar, jnp.maximum(steps - 1, 0)), 1.0)[:, None]
    return denoise(sample, eps, noise, now, before)


def denoise(sample, eps, noise, now, before):
    beta_prod = 1.0 - now
    cur_alpha = now / before
    cur_beta = 1.0 - cur_alpha
    start = jnp.clip((sample - jnp.sqrt(beta_prod) * eps) / jnp.sqrt(now), -1.0, 1.0)
    mean = (
        jnp.sqrt(before) * cur_beta / beta_prod * start
        + jnp.sqrt(cur_alpha) * (1.0 - before) / beta_prod * sample
    )
    spread = jnp.sqrt((1.0 - before) / beta_prod * cur_beta)
    return mean + spread * noise


DEPTH_PARTS = 4
PARTS = 2
VMEM = 60 * 1024 * 1024


def first_kernel(blocks, x_ref, wt_ref, cond_ref, film_ref, gain_ref, out_ref):
    x = x_ref[...]
    hs = [
        jnp.dot(x, wt_ref[h], preferred_element_type=jnp.float32) for h in range(HORIZON)
    ]
    width = hs[0].shape[1]
    count = HORIZON * width
    mean = sum(jnp.sum(h, axis=1, keepdims=True) for h in hs) / count
    hs = [h - mean for h in hs]
    var = sum(jnp.sum(h * h, axis=1, keepdims=True) for h in hs) / count
    inv = 1.0 / jnp.sqrt(var + 1e-05)
    cond = cond_ref[...]
    scale = jnp.dot(cond, film_ref[0], preferred_element_type=jnp.float32)
    shift = jnp.dot(cond, film_ref[1], preferred_element_type=jnp.float32)
    gain = gain_ref[...]
    cl = width // blocks
    for h in range(HORIZON):
        val = (scale * mish(hs[h] * inv * gain) + shift).astype(jnp.bfloat16)
        for b in range(blocks):
            out_ref[b, :, h * cl : (h + 1) * cl] = val[:, b * cl : (b + 1) * cl]


def first_stage(xs, wt, cond, film, gain, blocks, cl):
    rows = xs.shape[0]
    width = wt.shape[2]
    gw = C // GROUPS
    per = gw // cl
    rt = min(128, rows)
    inner = cond.shape[1]
    kern = lambda *refs: first_kernel(per, *refs)
    return pl.pallas_call(
        kern,
        grid=(width // gw, rows // rt),
        in_specs=[
            pl.BlockSpec((rt, xs.shape[1]), lambda g, r: (r, 0)),
            pl.BlockSpec((HORIZON, wt.shape[1], gw), lambda g, r: (0, 0, g)),
            pl.BlockSpec((rt, inner), lambda g, r: (r, 0)),
            pl.BlockSpec((2, inner, gw), lambda g, r: (0, 0, g)),
            pl.BlockSpec((1, gw), lambda g, r: (0, g)),
        ],
        out_specs=pl.BlockSpec((per, rt, HORIZON * cl), lambda g, r: (g, r, 0)),
        out_shape=jax.ShapeDtypeStruct((blocks, rows, HORIZON * cl), jnp.bfloat16),
        compiler_params=pltpu.CompilerParams(vmem_limit_bytes=VMEM),
        cost_estimate=pl.CostEstimate(
            flops=4 * rows * inner * width,
            bytes_accessed=4 * inner * width + 2 * rows * width * HORIZON,
            transcendentals=rows * width * HORIZON,
        ),
        name="first_stage",
    )(xs, wt, cond, film, gain)


def mix_kernel(pieces, mid, order_ref, *refs):
    a_ref, w_refs, out_ref = refs[0], refs[1 : 1 + pieces], refs[1 + pieces]
    cl = w_refs[0].shape[0] // TAPS
    parts, _, rows, _ = out_ref.shape
    for h in range(HORIZON):
        p0 = max(0, h - mid)
        p1 = min(HORIZON, h - mid + TAPS)
        k0 = p0 - h + mid
        k1 = p1 - h + mid
        acc = None
        for i in range(pieces):
            left = a_ref[order_ref[i], :, p0 * cl : p1 * cl]
            term = jnp.dot(
                left, w_refs[i][k0 * cl : k1 * cl, :], preferred_element_type=jnp.float32
            )
            acc = term if acc is None else acc + term
        for q in range(parts):
            out_ref[q, h] = acc[q * rows : (q + 1) * rows].astype(jnp.bfloat16)


def mix(order, acts, pieces):
    n = len(pieces)
    rows = acts.shape[1]
    width = pieces[0].shape[1]
    nt = min(256, width)
    kern = lambda *refs: mix_kernel(n, TAPS // 2, *refs)
    return pl.pallas_call(
        kern,
        grid=(width // nt,),
        in_specs=[
            pl.BlockSpec(memory_space=pltpu.SMEM),
            pl.BlockSpec(acts.shape, lambda j: (0, 0, 0)),
        ]
        + [pl.BlockSpec((p.shape[0], nt), lambda j: (0, j)) for p in pieces],
        out_specs=pl.BlockSpec(
            (DEPTH_PARTS, HORIZON, rows // DEPTH_PARTS, nt), lambda j: (0, 0, 0, j)
        ),
        out_shape=jax.ShapeDtypeStruct(
            (DEPTH_PARTS, HORIZON, rows // DEPTH_PARTS, width), jnp.bfloat16
        ),
        compiler_params=pltpu.CompilerParams(vmem_limit_bytes=VMEM),
        cost_estimate=pl.CostEstimate(
            flops=2 * 14 * rows * n * pieces[0].shape[0] // TAPS * width,
            bytes_accessed=2 * n * pieces[0].shape[0] * width + 8 * rows * width,
            transcendentals=0,
        ),
        name="mix",
    )(order, acts, *pieces)


def hop(value, axis, step):
    size = lax.axis_size(axis)
    return lax.ppermute(value, axis, [(i, (i + step) % size) for i in range(size)])


def relative(value):
    return jnp.concatenate(
        [value] + [hop(value, "z", -q) for q in range(1, DEPTH_PARTS)], axis=0
    )


def reduce_parts(part):
    half = HORIZON // 2
    far = part[2]
    up = hop(far[:half], "z", 1)
    down = hop(far[half:], "z", -1)
    f32 = jnp.float32
    near_up = (part[1, :half].astype(f32) + up.astype(f32)).astype(jnp.bfloat16)
    near_down = (part[3, half:].astype(f32) + down.astype(f32)).astype(jnp.bfloat16)
    got = [
        (hop(near_up, "z", 1), hop(part[3, :half], "z", -1)),
        (hop(part[1, half:], "z", 1), hop(near_down, "z", -1)),
    ]
    out = []
    for h in range(HORIZON):
        one, two = got[h // half]
        out.append(
            part[0, h].astype(f32) + one[h % half].astype(f32) + two[h % half].astype(f32)
        )
    return out


def general_body(
    noisy_sample,
    timestep,
    noise,
    obs_feat,
    step_w1,
    step_w2,
    film_weight,
    conv_in_w,
    residual_w,
    conv_mid_w,
    out_w,
    gain_one,
    gain_two,
):
    count = noisy_sample.shape[0]
    local_width = conv_in_w.shape[2]
    cl = conv_mid_w.shape[1]
    yn = lax.axis_size("y")
    zi, yi, ci = lax.axis_index("z"), lax.axis_index("y"), lax.axis_index("c")
    blocks = yn * 2
    kw = cl * blocks
    step = local_width // PARTS
    pieces = []
    for n in range(PARTS):
        own = conv_mid_w.reshape(TAPS * cl, local_width)[:, n * step : (n + 1) * step]
        near = [own] + [hop(own, "y", -s) for s in range(1, yn)]
        pieces.append(near + [hop(v, "c", 1) for v in near])
    order = jnp.stack(
        [((yi + s) % yn) * 2 + ci for s in range(yn)]
        + [((yi + s) % yn) * 2 + (1 - ci) for s in range(yn)]
    ).astype(jnp.int32)
    film = jnp.transpose(film_weight, (1, 0, 2))
    film = lax.all_gather(film, "tensor", axis=2, tiled=True)
    film = lax.all_to_all(film, "z", split_axis=2, concat_axis=1, tiled=True)
    film = lax.all_gather(film, ("y", "c"), axis=1, tiled=True)
    win = lax.all_gather(conv_in_w, "tensor", axis=2, tiled=True)
    win = lax.dynamic_slice_in_dim(win, zi * kw, kw, 2)
    gain = lax.all_gather(gain_one, "tensor", axis=0, tiled=True)
    gain = lax.dynamic_slice_in_dim(gain, zi * kw, kw, 0)[None, :]
    toep = []
    for h in range(HORIZON):
        rows = []
        for p in range(HORIZON):
            k = p - h + TAPS // 2
            rows.append(win[k] if 0 <= k < TAPS else jnp.zeros((ACT, kw), win.dtype))
        toep.append(jnp.concatenate(rows, axis=0))
    toep = jnp.stack(toep)
    sample_b = noisy_sample.astype(jnp.bfloat16)
    sinus = sinusoid(timestep).astype(jnp.bfloat16)
    step_hidden = mish(jnp.dot(sinus, step_w1, preferred_element_type=jnp.float32)).astype(
        jnp.bfloat16
    )
    step_feat = jnp.dot(step_hidden, step_w2, preferred_element_type=jnp.float32)
    cond = mish(jnp.concatenate([step_feat, obs_feat.astype(jnp.float32)], axis=1)).astype(
        jnp.bfloat16
    )
    fr = film_weight.shape[0]
    cond = (
        cond.reshape(count, DEPTH_PARTS, blocks, fr)
        .transpose(0, 2, 1, 3)
        .reshape(count, cond.shape[1])
    )
    acts = first_stage(relative(sample_b), toep, relative(cond), film, gain, blocks, cl)
    found = [reduce_parts(mix(order, acts, p)) for p in pieces]
    hs = [jnp.concatenate([f[h] for f in found], axis=1) for h in range(HORIZON)]
    gw = C // GROUPS
    outs = []
    cols = [slice(g * gw, (g + 1) * gw) for g in range(local_width // gw)]
    stats = []
    for col in cols:
        mean = sum(jnp.sum(h[:, col], axis=1, keepdims=True) for h in hs) / (HORIZON * gw)
        var = sum(jnp.sum((h[:, col] - mean) ** 2, axis=1, keepdims=True) for h in hs) / (
            HORIZON * gw
        )
        stats.append((mean, 1.0 / jnp.sqrt(var + 1e-05)))
    mean = jnp.concatenate([jnp.broadcast_to(m, (count, gw)) for m, _ in stats], axis=1)
    inv = jnp.concatenate([jnp.broadcast_to(v, (count, gw)) for _, v in stats], axis=1)
    for h in range(HORIZON):
        skip = jnp.dot(
            sample_b[:, h * ACT : (h + 1) * ACT], residual_w, preferred_element_type=jnp.float32
        )
        normed = (hs[h] - mean) * inv * gain_two[None, :]
        act_two = (mish(normed) + skip).astype(jnp.bfloat16)
        outs.append(jnp.dot(act_two, out_w, preferred_element_type=jnp.float32))
    eps = lax.psum(jnp.concatenate(outs, axis=1), "tensor")
    denoised = denoise_step(noisy_sample, eps, noise, timestep)
    return (eps, denoised)


CHUNK = 256
SPLIT = 2
LANES = 128
MESH_ID = pl.DeviceIdType.MESH


def remote(src, dst, send, recv, where):
    return pltpu.make_async_remote_copy(
        src_ref=src,
        dst_ref=dst,
        send_sem=send,
        recv_sem=recv,
        device_id=where,
        device_id_type=MESH_ID,
    )


def normed(hs, gain):
    count = len(hs) * hs[0].shape[1]
    mean = sum(jnp.sum(h, axis=1, keepdims=True) for h in hs) / count
    hs = [h - mean for h in hs]
    var = sum(jnp.sum(h * h, axis=1, keepdims=True) for h in hs) / count
    inv = 1.0 / jnp.sqrt(var + 1e-05)
    return [h * inv * gain for h in hs]


def fused_kernel(
    steps_ref,
    obs_ref,
    samp_ref,
    w1_ref,
    w2_ref,
    film_ref,
    conv_ref,
    gain_one_ref,
    mid_ref,
    skip_ref,
    outw_ref,
    gain_two_ref,
    sel_ref,
    noise_ref,
    table_ref,
    out_ref,
    square,
    w_buf,
    a_buf,
    film_buf,
    stage_buf,
    cond_buf,
    conv_buf,
    toep_buf,
    res_buf,
    gain_buf,
    own_part,
    z_recv,
    z_send,
    last,
    eps_acc,
    eps_send,
    eps_recv,
    own_sem,
    core_send,
    core_recv,
    y_send,
    y_recv,
    fwd_send,
    fwd_recv,
    stage_send,
    stage_recv,
    film_send,
    film_recv,
    filmy_send,
    filmy_recv,
    filmx_send,
    filmx_recv,
    filmc_send,
    filmc_recv,
    toep_send,
    toep_recv,
    cond_send,
    cond_recv,
    pair_send,
    pair_recv,
    condx_send,
    condx_recv,
    zs_sem,
    zr_sem,
    eps_ssem,
    eps_rsem,
):
    zi, yi = lax.axis_index("z"), lax.axis_index("y")
    ci, xi = lax.axis_index("c"), lax.axis_index("tensor")
    zn = DEPTH_PARTS
    f32, b16 = jnp.float32, jnp.bfloat16
    chunks = w_buf.shape[0]
    cl = w_buf.shape[2] // TAPS
    rows = obs_ref.shape[0]
    gw = C // GROUPS
    width = mid_ref.shape[1]
    kw = film_buf.shape[5]
    feat = w2_ref.shape[1] + obs_ref.shape[1]
    mid = TAPS // 2
    oy, oc, ox = 1 - yi, 1 - ci, 1 - xi
    to_y, to_c, to_x = {"y": oy}, {"c": oc}, {"tensor": ox}

    barrier = pltpu.get_barrier_semaphore()
    peers = [to_y, to_c]
    for dz in range(zn):
        for dx in range(2):
            if dz or dx:
                peers.append({"z": lax.rem(zi + dz, zn), "tensor": lax.rem(xi + dx, 2)})
    for peer in peers:
        pl.semaphore_signal(barrier, inc=1, device_id=peer, device_id_type=MESH_ID)

    def cols(j):
        return pl.ds(pl.multiple_of(j * CHUNK, CHUNK), CHUNK)

    def own_copy(j):
        return pltpu.make_async_copy(mid_ref.at[:, cols(j)], w_buf.at[j, 0], own_sem.at[j])

    def core_copy(j):
        return remote(
            mid_ref.at[:, cols(j)], w_buf.at[j, 1], core_send.at[j], core_recv.at[j], to_c
        )

    def y_half(j, i):
        some = pl.ds(i * (w_buf.shape[2] // 2), w_buf.shape[2] // 2)
        return remote(
            mid_ref.at[some, cols(j)],
            w_buf.at[j, 2, some],
            y_send.at[j, i],
            y_recv.at[j, i],
            to_y,
        )

    def fwd_copy(j):
        return remote(w_buf.at[j, 2], w_buf.at[j, 3], fwd_send.at[j], fwd_recv.at[j], to_c)

    near = [zi, zi + 1 - 2 * lax.rem(zi, 2), lax.rem(zi + 2, zn), zn - 1 - zi]
    home = zi // 2

    def half_cols(q):
        return pl.ds(pl.multiple_of(q * kw, kw), kw)

    def stage_copy(q):
        return remote(
            film_ref.at[ox, :, half_cols(q)],
            stage_buf.at[q],
            stage_send.at[q],
            stage_recv.at[q],
            to_x,
        )

    def plane_copy():
        return remote(
            film_ref.at[ox, :, half_cols(lax.rem(zi, 2))],
            film_buf.at[ox, zi, yi, ci],
            stage_send.at[lax.rem(zi, 2)],
            film_recv.at[zi],
            to_x,
        )

    def film_own(q):
        return remote(
            film_ref.at[xi, :, half_cols(q)],
            film_buf.at[xi, zi, yi, ci],
            film_send.at[0, q],
            film_recv.at[zi],
            {"z": 2 * xi + q},
        )

    def film_staged(q):
        return remote(
            stage_buf.at[q],
            film_buf.at[xi, zi, yi, ci],
            film_send.at[1, q],
            film_recv.at[zi],
            {"z": 2 * ox + q},
        )

    pl.semaphore_wait(barrier, len(peers))
    for q in range(2):
        mine = 2 * xi + q == zi

        @pl.when(mine)
        def _():
            plane_copy().start()
            pltpu.make_async_copy(
                film_ref.at[xi, :, half_cols(q)], film_buf.at[xi, zi, yi, ci], film_recv.at[zi]
            ).start()

        @pl.when(jnp.logical_not(mine))
        def _():
            stage_copy(q).start()
            film_own(q).start()

    y_half(0, 0).start()

    @pl.loop(0, chunks)
    def _(j):
        own_copy(j).start()
        core_copy(j).start()

    at = half_cols(lax.rem(zi, 2))

    def conv_copy():
        return remote(conv_ref.at[:, :, at], conv_buf, toep_send.at[0], toep_recv.at[0], to_x)

    def gain_copy():
        return remote(gain_one_ref.at[:, at], gain_buf, toep_send.at[1], toep_recv.at[1], to_x)

    @pl.when(xi == home)
    def _():
        conv_copy().start()
        gain_copy().start()
        pltpu.make_async_copy(conv_ref.at[:, :, at], conv_buf, toep_recv.at[0]).start()
        pltpu.make_async_copy(gain_one_ref.at[:, at], gain_buf, toep_recv.at[1]).start()

    half = rows // 2
    sw = w2_ref.shape[1]
    cond_obs = mish(obs_ref[...].astype(f32)).astype(b16)
    square[...] = jnp.zeros_like(square)
    square[: HORIZON * ACT] = samp_ref[...]
    samp = square[...].T.astype(b16)
    count = w1_ref.shape[0] // 2
    index = lax.broadcasted_iota(jnp.int32, (count, rows), 0).astype(f32)
    freqs = jnp.exp(index * (-math.log(10000.0) / (count - 1)))
    angles = steps_ref[...].astype(f32) * freqs
    sinus = jnp.concatenate([jnp.sin(angles), jnp.cos(angles)], axis=0).astype(b16)
    hidden = mish(
        lax.dot_general(
            sinus, w1_ref[...], (((0,), (0,)), ((), ())), preferred_element_type=f32
        )
    ).astype(b16)
    step_feat = jnp.dot(hidden, w2_ref[...], preferred_element_type=f32)
    cond_step = mish(step_feat).astype(b16)
    for i in range(2):
        part = slice(i * half, (i + 1) * half)
        cond_buf[zi, i, :, :sw] = cond_step[part]
        cond_buf[zi, i, :, sw:feat] = cond_obs[part]
        cond_buf[zi, i, :, feat:] = samp[part]

    def cond_copy(dz):
        return remote(
            cond_buf.at[zi, xi],
            cond_buf.at[zi, xi],
            cond_send.at[dz - 2],
            cond_recv.at[zi],
            {"z": near[dz]},
        )

    def condx_copy(z, i):
        return remote(
            cond_buf.at[z, i], cond_buf.at[z, i], condx_send.at[z], condx_recv.at[z], to_x
        )

    def cond_in(z):
        return remote(
            cond_buf.at[z, xi], cond_buf.at[z, xi], cond_send.at[0], cond_recv.at[z], to_x
        )

    def film_in(z):
        piece = film_buf.at[xi, z, yi, ci]
        return remote(piece, piece, film_send.at[0, 0], film_recv.at[z], to_x)

    def film_y(z, t, y):
        piece = film_buf.at[t, z, y, ci]
        return remote(piece, piece, filmy_send.at[z], filmy_recv.at[z], to_y)

    def film_x(z, t, y):
        piece = film_buf.at[t, z, y, ci]
        k = (y + yi) % 2
        return remote(piece, piece, filmx_send.at[k, z], filmx_recv.at[k, z], to_x)

    def film_c(z, t, y, c):
        piece = film_buf.at[t, z, y, c]
        k = 2 * ((t + xi) % 2) + (y + yi) % 2
        return remote(piece, piece, filmc_send.at[k, z], filmc_recv.at[k, z], to_c)

    def arrived(z):
        film_in(z).wait_recv()
        film_y(z, xi, yi).start()
        film_x(z, xi, yi).start()
        film_c(z, xi, yi, ci).start()

    def crossed(z):
        film_y(z, xi, oy).wait_recv()
        film_x(z, xi, oy).start()
        film_c(z, xi, oy, ci).start()

    def known(z):
        cond_in(z).wait_recv()
        condx_copy(z, xi).start()

    arrived(near[0])
    y_half(0, 1).start()

    for q in range(2):

        @pl.when(2 * ox + q != zi)
        def _():
            stage_copy(q).wait_recv()
            film_staged(q).start()

    def cond_pair(i):
        return remote(
            cond_buf.at[zi, i],
            cond_buf.at[zi, i],
            pair_send.at[i],
            pair_recv.at[i],
            {"z": near[1]},
        )

    for i in range(2):
        cond_pair(i).start()
    for k in range(2, zn):
        cond_copy(k).start()

    arrived(near[1])
    crossed(near[0])
    arrived(near[2])
    crossed(near[1])
    y_half(1, 0).start()
    arrived(near[3])
    y_half(1, 1).start()
    crossed(near[2])

    @pl.loop(2, chunks)
    def _(j):
        for i in range(2):
            y_half(j, i).start()

    known(near[2])
    crossed(near[3])
    known(near[3])
    conv_copy().wait_recv()
    gain_copy().wait_recv()
    total = None
    for k in range(TAPS):
        term = jnp.dot(sel_ref[k], conv_buf[k], preferred_element_type=f32)
        total = term if total is None else total + term
    toep_buf[...] = total.astype(b16)
    res_buf[...] = jnp.dot(sel_ref[mid], skip_ref[...], preferred_element_type=f32).astype(b16)
    for z in near:
        film_x(z, ox, yi).wait_recv()
        film_c(z, ox, yi, ci).start()
    for z in near:
        film_x(z, ox, oy).wait_recv()
        film_c(z, ox, oy, ci).start()
    for z in near[2:]:
        condx_copy(z, ox).wait_recv()
    for i in range(2):
        piece = cond_buf.at[near[1], i]
        remote(piece, piece, pair_send.at[i], pair_recv.at[i], to_x).wait_recv()
    for z in near:
        for t in range(2):
            for y in range(2):
                film_c(z, t, y, oc).wait_recv()

    per = gw // cl
    inner = film_buf.shape[1] * film_buf.shape[2] * film_buf.shape[3] * film_buf.shape[4]
    pad = sel_ref.shape[1] // HORIZON

    def first(r, ab):
        z = ab * SPLIT + r
        cond = cond_buf[z].reshape(rows, cond_buf.shape[3])
        x = cond[:, feat : feat + pad]
        cond = cond[:, :feat]
        for g in range(kw // gw):
            span = slice(g * gw, (g + 1) * gw)
            hs = [
                jnp.dot(
                    x, toep_buf[h * pad : (h + 1) * pad, span], preferred_element_type=f32
                )
                for h in range(HORIZON)
            ]
            hs = normed(hs, gain_buf[0:1, span])
            scale = jnp.dot(
                cond,
                film_buf[0, :, :, :, :, span].reshape(inner, gw),
                preferred_element_type=f32,
            )
            shift = jnp.dot(
                cond,
                film_buf[1, :, :, :, :, span].reshape(inner, gw),
                preferred_element_type=f32,
            )
            for h in range(HORIZON):
                val = (scale * mish(hs[h]) + shift).astype(b16)
                for b in range(per):
                    a_buf[g * per + b, r, ab, :, h * cl : (h + 1) * cl] = val[
                        :, b * cl : (b + 1) * cl
                    ]

    eps_acc[...] = jnp.zeros_like(eps_acc)
    order = [yi * 2 + ci, yi * 2 + oc, oy * 2 + ci, oy * 2 + oc]
    steps = chunks * SPLIT
    ring = own_part.shape[0]
    zring = z_send.shape[1]
    ends = (zi == 0) | (zi == zn - 1)

    def z_copy(d, s, h):
        k = lax.rem(s, zring)
        return remote(
            z_send.at[d, k, h],
            z_recv.at[d, s, h],
            zs_sem.at[d, k, h],
            zr_sem.at[d, s, h],
            {"z": jnp.maximum(zi - 1, 0) if d == 0 else jnp.minimum(zi + 1, zn - 1)},
        )

    def flow(d, now):
        pos = zn - 1 - zi if d == 0 else zi
        s = now - pos - pos // (zn - 1)
        k = lax.rem(s + ring, ring)
        kz = lax.rem(s + zring, zring)

        @pl.when((s >= 0) & (s < steps))
        def _():
            @pl.when(pos == zn - 1)
            def _():
                for h in range(HORIZON):
                    z_copy(d, s, h).wait_recv()
                    last[lax.rem(s, SPLIT), lax.rem(s // SPLIT, 2), h] = own_part[
                        k, d, h
                    ] + z_recv[d, s, h].astype(f32)

            @pl.when((pos < zn - 1) & (s >= zring))
            def _():
                for h in range(HORIZON):
                    z_copy(d, s - zring, h).wait_send()

            @pl.when(pos == 0)
            def _():
                for h in range(HORIZON):
                    z_send[d, kz, h] = own_part[k, d, h].astype(b16)
                    z_copy(d, s, h).start()

            @pl.when((pos > 0) & (pos < zn - 1))
            def _():
                for h in range(HORIZON):
                    z_copy(d, s, h).wait_recv()
                    z_send[d, kz, h] = (
                        own_part[k, d, h] + z_recv[d, s, h].astype(f32)
                    ).astype(b16)
                    z_copy(d, s, h).start()

    @pl.loop(0, steps + zn)
    def _(now):
        @pl.when(now < SPLIT)
        def _():
            @pl.loop(0, 2)
            def _(ab):
                first(now, ab)

        @pl.when(now < steps)
        def _():
            j = now // SPLIT
            r = lax.rem(now, SPLIT)
            k = lax.rem(now, ring)

            @pl.when(r == 0)
            def _():
                for i in range(2):
                    y_half(j, i).wait_recv()
                fwd_copy(j).start()
                own_copy(j).wait()
                core_copy(j).wait_recv()
                fwd_copy(j).wait_recv()

            for h in range(HORIZON):
                p0 = max(0, h - mid)
                p1 = min(HORIZON, h - mid + TAPS)
                k0 = p0 - h + mid
                k1 = p1 - h + mid
                acc = None
                for slot in range(4):
                    left = a_buf[order[slot], r, :, :, p0 * cl : p1 * cl]
                    term = jnp.dot(
                        left.reshape(2 * rows, (p1 - p0) * cl),
                        w_buf[j, slot, k0 * cl : k1 * cl, :],
                        preferred_element_type=f32,
                    )
                    acc = term if acc is None else acc + term
                for d in range(2):
                    own_part[k, d, h] = acc[d * rows : (d + 1) * rows]

        @pl.when(zi < zn // 2)
        def _():
            flow(1, now)

        flow(0, now)

        @pl.when(zi >= zn // 2)
        def _():
            flow(1, now)

        done = now - zn

        @pl.when((done >= 0) & ends & (lax.rem(done // SPLIT, 2) == 1))
        def _():
            r = lax.rem(done, SPLIT)
            g = done // (2 * SPLIT)
            z = (zi // (zn - 1)) * SPLIT + r
            span = pl.ds(pl.multiple_of(g * gw, gw), gw)
            hs = [
                jnp.concatenate([last[r, 0, h], last[r, 1, h]], axis=1) for h in range(HORIZON)
            ]
            hs = normed(hs, gain_two_ref[0:1, span])
            x = cond_buf[z, :, :, feat:].reshape(rows, LANES)[:, :pad]
            for h in range(HORIZON):
                skip = jnp.dot(
                    x, res_buf[h * pad : (h + 1) * pad, span], preferred_element_type=f32
                )
                act = (mish(hs[h]) + skip).astype(b16)
                eps_acc[r, h] += lax.dot_general(
                    act,
                    outw_ref[:, span],
                    (((1,), (1,)), ((), ())),
                    preferred_element_type=f32,
                )

    end = (zi // SPLIT) * (zn - 1)

    def eps_copy(r, t):
        return remote(
            eps_send.at[r],
            eps_recv.at[xi],
            eps_ssem.at[r, t],
            eps_rsem.at[xi],
            {"z": (zi // (zn - 1)) * SPLIT + r, "tensor": t},
        )

    for r in range(SPLIT):
        z = (zi // (zn - 1)) * SPLIT + r

        @pl.when(ends)
        def _():
            total = jnp.concatenate(
                [eps_acc[r, h] for h in range(HORIZON)]
                + [jnp.zeros((rows, LANES - HORIZON * ACT), f32)],
                axis=1,
            )
            total = total.T[: eps_send.shape[1]]
            eps_send[r] = total

            @pl.when(z == zi)
            def _():
                eps_recv[xi] = total

            for t in range(2):

                @pl.when((z != zi) | (xi != t))
                def _():
                    eps_copy(r, t).start()

    for t in range(2):

        @pl.when((zi != end) | (xi != t))
        def _():
            remote(
                eps_send.at[0], eps_recv.at[t], eps_ssem.at[0, 0], eps_rsem.at[t], to_x
            ).wait_recv()

    eps = (eps_recv[0] + eps_recv[1])[: HORIZON * ACT]
    out_ref[0, : HORIZON * ACT] = eps
    when = steps_ref[...]
    spots = lax.broadcasted_iota(jnp.int32, square.shape, 0)
    table = jnp.broadcast_to(table_ref[...], square.shape).T
    now = jnp.sum(jnp.where(spots == when, table, 0.0), axis=0, keepdims=True)
    before = jnp.sum(jnp.where(spots == when - 1, table, 0.0), axis=0, keepdims=True)
    before = jnp.where(when > 0, before, 1.0)
    out_ref[1, : HORIZON * ACT] = denoise(samp_ref[...], eps, noise_ref[...], now, before)

    for r in range(SPLIT):
        z = (zi // (zn - 1)) * SPLIT + r
        for t in range(2):

            @pl.when(ends & ((z != zi) | (xi != t)))
            def _():
                eps_copy(r, t).wait_send()

    for d in range(2):

        @pl.when((zi < zn - 1) if d else (zi > 0))
        def _():
            for s in range(steps - zring, steps):
                for h in range(HORIZON):
                    z_copy(d, s, h).wait_send()

    @pl.loop(0, chunks)
    def _(j):
        for i in range(2):
            y_half(j, i).wait_send()
        core_copy(j).wait_send()
        fwd_copy(j).wait_send()

    for q in range(2):
        mine = 2 * xi + q == zi

        @pl.when(mine)
        def _():
            plane_copy().wait_send()

        @pl.when(jnp.logical_not(mine))
        def _():
            stage_copy(q).wait_send()
            film_own(q).wait_send()

        @pl.when(2 * ox + q != zi)
        def _():
            film_staged(q).wait_send()

    @pl.when(xi == home)
    def _():
        conv_copy().wait_send()
        gain_copy().wait_send()

    for i in range(2):
        cond_pair(i).wait_send()
    for k in range(2, zn):
        cond_copy(k).wait_send()
        condx_copy(near[k], xi).wait_send()
    for z in near:
        film_y(z, xi, yi).wait_send()
        film_x(z, xi, yi).wait_send()
        film_x(z, xi, oy).wait_send()
        for y in range(2):
            for t in range(2):
                film_c(z, t, y, ci).wait_send()


def fused(steps, obs, samp, w1, w2, film, conv, gain_one, weights, skip, outw, gain_two, sel, noise, table):
    rows = obs.shape[0]
    depth, width = weights.shape
    chunks = width // CHUNK
    cl = depth // TAPS
    kw = cl * 4
    fr = film.shape[1]
    feat = w2.shape[1] + obs.shape[1]
    count = chunks * SPLIT
    ring = DEPTH_PARTS + 1
    zring = 4
    b16, f32 = jnp.bfloat16, jnp.float32
    dma = pltpu.SemaphoreType.DMA
    vm = pl.BlockSpec(memory_space=pltpu.VMEM)
    hbm = pl.BlockSpec(memory_space=pl.ANY)
    return pl.pallas_call(
        fused_kernel,
        out_shape=jax.ShapeDtypeStruct((2, 32, rows), f32),
        in_specs=[vm, vm, vm, vm, vm, hbm, hbm, hbm, hbm, vm, vm, vm, vm, vm, vm],
        out_specs=vm,
        scratch_shapes=[
            pltpu.VMEM((LANES, LANES), f32),
            pltpu.VMEM((chunks, 4, depth, CHUNK), b16),
            pltpu.VMEM((4, SPLIT, 2, rows, HORIZON * cl), b16),
            pltpu.VMEM((2, DEPTH_PARTS, 2, 2, fr, kw), b16),
            pltpu.VMEM((2, fr, kw), b16),
            pltpu.VMEM((DEPTH_PARTS, 2, rows // 2, feat + LANES), b16),
            pltpu.VMEM((TAPS, ACT, kw), b16),
            pltpu.VMEM((sel.shape[1], kw), b16),
            pltpu.VMEM((sel.shape[1], width), b16),
            pltpu.VMEM((gain_one.shape[0], kw), f32),
            pltpu.VMEM((ring, 2, HORIZON, rows, CHUNK), f32),
            pltpu.VMEM((2, count, HORIZON, rows, CHUNK), b16),
            pltpu.VMEM((2, zring, HORIZON, rows, CHUNK), b16),
            pltpu.VMEM((SPLIT, 2, HORIZON, rows, CHUNK), f32),
            pltpu.VMEM((SPLIT, HORIZON, rows, ACT), f32),
            pltpu.VMEM((SPLIT, 32, rows), f32),
            pltpu.VMEM((2, 32, rows), f32),
            dma((chunks,)),
            dma((chunks,)),
            dma((chunks,)),
            dma((chunks, 2)),
            dma((chunks, 2)),
            dma((chunks,)),
            dma((chunks,)),
            dma((2,)),
            dma((2,)),
            dma((2, 2)),
            dma((DEPTH_PARTS,)),
            dma((DEPTH_PARTS,)),
            dma((DEPTH_PARTS,)),
            dma((2, DEPTH_PARTS)),
            dma((2, DEPTH_PARTS)),
            dma((4, DEPTH_PARTS)),
            dma((4, DEPTH_PARTS)),
            dma((2,)),
            dma((2,)),
            dma((DEPTH_PARTS - 2,)),
            dma((DEPTH_PARTS,)),
            dma((2,)),
            dma((2,)),
            dma((DEPTH_PARTS,)),
            dma((DEPTH_PARTS,)),
            dma((2, zring, HORIZON)),
            dma((2, count, HORIZON)),
            dma((SPLIT, 2)),
            dma((2,)),
        ],
        compiler_params=pltpu.CompilerParams(
            collective_id=0, has_side_effects=True, vmem_limit_bytes=VMEM
        ),
        name="fused_step",
    )(steps, obs, samp, w1, w2, film, conv, gain_one, weights, skip, outw, gain_two, sel, noise, table)


def selection(dtype):
    pad = 32
    table = np.zeros((TAPS, HORIZON * pad, ACT), np.float32)
    for h in range(HORIZON):
        for p in range(HORIZON):
            k = p - h + TAPS // 2
            for a in range(ACT):
                if 0 <= k < TAPS:
                    table[k, h * pad + p * ACT + a, a] = 1.0
    return jnp.asarray(table, dtype)


def fused_body(
    noisy_sample,
    timestep,
    noise,
    obs_feat,
    step_w1,
    step_w2,
    film_weight,
    conv_in_w,
    residual_w,
    conv_mid_w,
    out_w,
    gain_one,
    gain_two,
):
    width = conv_in_w.shape[2]
    table = plan()
    both = fused(
        timestep[None, :],
        obs_feat,
        noisy_sample.T,
        step_w1,
        step_w2,
        jnp.transpose(film_weight, (1, 0, 2)),
        conv_in_w,
        gain_one[None, :],
        conv_mid_w.reshape(-1, width),
        residual_w,
        out_w.T,
        gain_two[None, :],
        selection(conv_in_w.dtype),
        noise.T,
        jnp.pad(table, (0, LANES - table.shape[0]))[None, :],
    )
    return (both[0, : HORIZON * ACT].T, both[1, : HORIZON * ACT].T)


def solution(mesh):
    dp, tensor = mesh.shape["dp"], mesh.shape["tensor"]
    near = dp // DEPTH_PARTS // 2
    body = fused_body if near == 2 and tensor == 2 else general_body
    grid = Mesh(
        mesh.devices.reshape(DEPTH_PARTS, dp // DEPTH_PARTS // 2, 2, tensor),
        ("z", "y", "c", "tensor"),
    )
    rows = ("z", "y", "c")
    return jax.shard_map(
        body,
        mesh=grid,
        in_specs=(
            P(rows, None),
            P(rows),
            P(rows, None),
            P(rows, None),
            P(),
            P(),
            P(rows, None, "tensor"),
            P(None, None, "tensor"),
            P(None, "tensor"),
            P(None, rows, "tensor"),
            P("tensor", None),
            P("tensor"),
            P("tensor"),
        ),
        out_specs=(P(rows, None), P(rows, None)),
        check_vma=False,
    )
```
